32 devices in a mesh: dp: 4 (over y, core), fsdp: 8 (over z, x).
Axes of the slice: x: 2, y: 2, z: 4, core: 2. Of those that a mesh axis runs over, the one named last changes fastest.
Arguments:
- images: bfloat16 [192, 784, 320], P(('dp', 'fsdp')), may hold values from -50 to 50
- counts: int32 [32], P(('dp', 'fsdp')), may hold values from 1 to 6, 96 in all
- cotangent: bfloat16 [192, 784, 320], P(('dp', 'fsdp')), may hold values from -6 to 6
- master: float32 [1658880], P(('dp', 'fsdp')), may hold values from -4 to 4
- first_moment: float32 [1658880], P(('dp', 'fsdp')), may hold values from -219.47428 to 219.47428
- second_moment: float32 [1658880], P(('dp', 'fsdp')), may hold values from 737.5872 to 12268.032, as said below
- average: float32 [1658880], P(('dp', 'fsdp')), may hold values from -4 to 4
Outputs:
- grads: float32 [1658880], P(('dp', 'fsdp'))
- new_first: float32 [1658880], P(('dp', 'fsdp'))
- new_second: float32 [1658880], P(('dp', 'fsdp'))
- new_master: float32 [1658880], P(('dp', 'fsdp'))
- new_average: float32 [1658880], P(('dp', 'fsdp'))
- new_copy: bfloat16 [1658880], P(('dp', 'fsdp'))
- output_images: bfloat16 [192, 784, 320], P(('dp', 'fsdp'))
- grad_images: bfloat16 [192, 784, 320], P(('dp', 'fsdp'))
The draws below stay inside these ranges and needn't reach their ends.
Inputs may be any that keep to these rules, and one draw needn't show every extreme that they name: counts sum to 96; at least one device holds exactly 6. `second_moment`: positive.
All inputs are finite; a program needn't handle non-finite values.
Results may differ from the reference program's by a relative error of at most 0.013.
The reference program's roundings to bfloat16 on the way count: a program that leaves them out, or rounds other values in their place, can miss the bound.
Values may be sent and summed in bfloat16 or wider, within the bound.
A program may use at most 128 MiB of HBM per device.

```python
import math
import jax
import jax.numpy as jnp
import numpy as np
from jax import lax

C = 320
HEADS = 5
HEADSZ = 64
HID = 1280
SIDE = 28
STEP = 3
HALF = 14
NTOK = 784
KEYS = 196
CAP = 6
IMAGES = 96
SLOTS = 192
PCOUNT = 1656000
PARAMS = 1658880
DEVICES = 32


def segment_scales():
    return [('norm_gain', C, -1.0), ('norm_bias', C, 0.3), ('query_weight', C * C, 1.5 / math.sqrt(C)), ('query_bias', C, 0.3), ('reduce_weight', 4 * C * C, 1.0 / math.sqrt(4 * C)), ('reduce_bias', C, 0.3), ('keys_gain', C, -1.0), ('keys_bias', C, 0.3), ('kv_weight', 2 * C * C, 1.0 / math.sqrt(C)), ('value_bias', C, 0.3), ('out_weight', C * C, 4.0 / math.sqrt(C)), ('out_bias', C, 0.3), ('mlp_gain', C, -1.0), ('mlp_bias', C, 0.3), ('up_weight', C * HID, 1.0 / math.sqrt(C)), ('up_bias', HID, 0.3), ('depth_weight', 9 * HID, 1.0 / 3.0), ('depth_bias', HID, 0.3), ('down_weight', HID * C, 1.0 / math.sqrt(HID)), ('down_bias', C, 0.3)]


def base_noise(key, shape_dims):
    return jnp.clip(jax.random.normal(key, shape_dims, jnp.float32), -4.0, 4.0)


def parameter_vector(key):
    blocks = []
    for seg_index, seg_entry in enumerate(segment_scales()):
        noise = base_noise(jax.random.fold_in(key, seg_index), (seg_entry[1],))
        if seg_entry[2] < 0:
            blocks.append(1.0 + 0.15 * noise)
        else:
            blocks.append(seg_entry[2] * noise)
    blocks.append(0.02 * base_noise(jax.random.fold_in(key, 99), (PARAMS - PCOUNT,)))
    return jnp.concatenate(blocks)


def grad_scale():
    return 0.2 * math.sqrt(IMAGES * NTOK)


def draw_images(key, part):
    first_key = jax.random.fold_in(key, 1)
    row_key = jax.random.fold_in(key, 2)
    col_key = jax.random.fold_in(key, 3)
    rows_scale = jnp.exp(jax.random.uniform(row_key, (SLOTS, NTOK, 1), jnp.float32, -1.2, 1.2))
    cols_scale = jnp.exp(jax.random.uniform(col_key, (1, 1, C), jnp.float32, -1.2, 1.2))
    base_values = jnp.clip(jax.random.normal(first_key, (SLOTS, NTOK, C), jnp.float32), -4.0, 4.0)
    return (base_values * rows_scale * cols_scale).astype(jnp.bfloat16)


def draw_master(key, part):
    return parameter_vector(jax.random.fold_in(key, 11))


def draw_average(key, part):
    return parameter_vector(jax.random.fold_in(key, 23))


def draw_first_moment(key, part):
    return grad_scale() * base_noise(jax.random.fold_in(key, 31), (PARAMS,))


def draw_second_moment(key, part):
    spread = jnp.exp(jax.random.uniform(jax.random.fold_in(key, 41), (PARAMS,), jnp.float32, -0.7, 0.7))
    root_part = grad_scale() * spread
    return root_part * root_part


def levels(own_key, dims, cuts, smallest, high):
    level = 1.0
    for position, shards_of in cuts:
        steps = jax.random.uniform(jax.random.fold_in(jax.random.fold_in(own_key, 6), position), (shards_of,), jnp.float32, smallest / len(cuts), high / len(cuts))
        level = level * jnp.repeat(jnp.exp(steps), dims[position] // shards_of).reshape((-1,) + (1,) * (len(dims) - 1 - position))
    return level


def length_profile(count, total, most, skew):
    weights = [(1 << 20) // math.isqrt(rank ** skew) + 1 for rank in range(2, count + 1)]
    rest, holding = total - most - (count - 1), [1] * (count - 1)
    while rest > 0:
        movable = [i for i in range(count - 1) if holding[i] < most]
        mass, remaining = sum([weights[i] for i in movable]), rest
        for i in movable:
            more = min(most - holding[i], max(1, remaining * weights[i] // mass), rest)
            holding[i] = holding[i] + more
            rest = rest - more
    return np.array([most] + holding)


def uneven_parts(stream_key, amount, total, limit, lean):
    if amount == 2:
        one = jax.random.randint(stream_key, (), max(1, total - limit), min(limit, total - 1) + 1)
        return jnp.stack([one, total - one])
    sizes = jnp.asarray(length_profile(amount, total, limit, lean), jnp.int32)
    twos = (amount - 1) // 2
    donor, receiver = sizes[1:1 + 2 * twos:2], sizes[2:2 + 2 * twos:2]
    slack = jnp.minimum(donor - 1, limit - receiver)
    moved = jax.random.randint(jax.random.fold_in(stream_key, 1), (twos,), 0, 1 << 20) % (slack + 1)
    sizes = sizes.at[1:1 + 2 * twos:2].set(donor - moved).at[2:2 + 2 * twos:2].set(receiver + moved)
    return sizes[jax.random.permutation(jax.random.fold_in(stream_key, 2), amount)]


def bell_draw(rng, dims, width, limit, cuts=(), held_as=jnp.bfloat16):
    array = jax.random.normal(rng, dims, jnp.float32) * width
    if len(cuts) > 0:
        array = levels(rng, dims, cuts, -0.22, 0.18) * array
    return jnp.clip(array, min=-limit, max=limit).astype(held_as)


def setup_inputs(seed: int = 0) -> dict:
    key_of = jax.random.split(jax.random.key(seed), 8)
    images = draw_images(jax.random.fold_in(key_of[7], 71), 0)
    counts = uneven_parts(key_of[1], DEVICES, IMAGES, CAP, 2).astype(jnp.int32)
    cotangent = bell_draw(key_of[2], (SLOTS, NTOK, C), 1.0, 6.0, ((0, 32),))
    master = draw_master(jax.random.fold_in(key_of[7], 71), 0)
    first_moment = draw_first_moment(jax.random.fold_in(key_of[7], 71), 0)
    second_moment = draw_second_moment(jax.random.fold_in(key_of[7], 71), 0)
    average = draw_average(jax.random.fold_in(key_of[7], 71), 0)
    return dict(images=images, counts=counts, cotangent=cotangent, master=master, first_moment=first_moment, second_moment=second_moment, average=average)


@jax.custom_vjp
def low(v):
    return lax.optimization_barrier(v.astype(jnp.bfloat16)).astype(jnp.float32)

@jax.custom_vjp
def low_back(v):
    return v

def low_keep(v):
    return (low(v), None)

def low_pass(kept, grad):
    return (grad,)

def back_keep(v):
    return (v, None)

def back_low(kept, grad):
    return (low(grad),)
low.defvjp(low_keep, low_pass)
low_back.defvjp(back_keep, back_low)
norm_eps = 1e-06
adam_eps = 1e-08
learn_rate = 0.02
weight_decay = 0.05
beta_first = 0.5
beta_second = 0.5
ema_keep = 0.9

def segments():
    return [('norm_gain', (C,)), ('norm_bias', (C,)), ('query_weight', (C, C)), ('query_bias', (C,)), ('reduce_weight', (4 * C, C)), ('reduce_bias', (C,)), ('keys_gain', (C,)), ('keys_bias', (C,)), ('kv_weight', (C, 2 * C)), ('value_bias', (C,)), ('out_weight', (C, C)), ('out_bias', (C,)), ('mlp_gain', (C,)), ('mlp_bias', (C,)), ('up_weight', (C, HID)), ('up_bias', (HID,)), ('depth_weight', (9, HID)), ('depth_bias', (HID,)), ('down_weight', (HID, C)), ('down_bias', (C,))]

def unpack(flat_vector):
    pieces = {}
    offset = 0
    for seg_name, seg_shape in segments():
        seg_size = math.prod(seg_shape)
        pieces[seg_name] = flat_vector[offset:offset + seg_size].reshape(seg_shape)
        offset += seg_size
    return pieces

def layer_norm(values, gain_vec, bias_vec):
    centred = values - lax.optimization_barrier(jnp.mean(values, -1, keepdims=True))
    spread = lax.optimization_barrier(jnp.mean(centred * centred, -1, keepdims=True))
    return centred * lax.rsqrt(spread + norm_eps) * gain_vec + bias_vec

def matmul(left_side, right_side):
    return jnp.matmul(left_side, right_side, precision=lax.Precision.HIGHEST)

def to_patches(grid_rows):
    return grid_rows.reshape(HALF, 2, HALF, 2, C).transpose(0, 2, 1, 3, 4).reshape(KEYS, 4 * C)

def depthwise(values, tap_table, bias_vec):
    padded = jnp.pad(values.reshape(SIDE, SIDE, HID), ((1, 1), (1, 1), (0, 0)))
    result = jnp.zeros((SIDE, SIDE, HID), jnp.float32) + bias_vec
    for row_tap in range(3):
        for col_tap in range(3):
            result = result + padded[row_tap:row_tap + SIDE, col_tap:col_tap + SIDE] * tap_table[3 * row_tap + col_tap]
    return result.reshape(NTOK, HID)

def image_forward(weights, one_image):
    pieces = unpack(weights)
    hidden = low(layer_norm(one_image, pieces['norm_gain'], pieces['norm_bias']))
    queries = low(low_back(matmul(hidden, pieces['query_weight']) + pieces['query_bias']))
    reduced = low_back(matmul(to_patches(hidden), pieces['reduce_weight']) + pieces['reduce_bias'])
    normed = low(layer_norm(reduced, pieces['keys_gain'], pieces['keys_bias']))
    kv_bias = jnp.concatenate([jnp.zeros((C,), jnp.float32), pieces['value_bias']])
    keyval = low(low_back(matmul(normed, pieces['kv_weight']) + kv_bias))
    key_rows = keyval[:, :C].reshape(KEYS, HEADS, HEADSZ)
    values = keyval[:, C:].reshape(KEYS, HEADS, HEADSZ)
    scores = low_back(jnp.einsum('qhd,khd->hqk', queries.reshape(NTOK, HEADS, HEADSZ), key_rows, precision=lax.Precision.HIGHEST) * HEADSZ ** (-0.5))
    attention = low(jax.nn.softmax(scores, axis=-1))
    attended = jnp.einsum('hqk,khd->qhd', attention, values, precision=lax.Precision.HIGHEST).reshape(NTOK, C)
    attended = low(low_back(attended))
    middle = one_image + low_back(matmul(attended, pieces['out_weight']) + pieces['out_bias'])
    hidden_two = low(layer_norm(middle, pieces['mlp_gain'], pieces['mlp_bias']))
    expanded = low_back(matmul(hidden_two, pieces['up_weight']) + pieces['up_bias'])
    conv_out = depthwise(expanded, pieces['depth_weight'], pieces['depth_bias'])
    active = low(jax.nn.gelu(conv_out, approximate=False))
    return middle + low_back(matmul(active, pieces['down_weight']) + pieces['down_bias'])

def reference(images, counts, cotangent, master, first_moment, second_moment, average):
    weights = master.astype(jnp.bfloat16).astype(jnp.float32)
    live_slots = jnp.arange(SLOTS) % CAP < jnp.repeat(counts, CAP)
    checked = jax.checkpoint(image_forward)

    def loss_total(weights_in, images_in):

        def scan_step(running, scan_item):
            image_row, target_grad, alive = scan_item
            result = lax.cond(alive, lambda image_arg: checked(weights_in, image_arg), lambda image_arg: jnp.zeros_like(image_arg), image_row)
            return (running + jnp.sum(result * target_grad), result)
        return lax.scan(scan_step, jnp.zeros((), jnp.float32), (images_in, cotangent.astype(jnp.float32), live_slots))
    (loss_value, out_images), pullback = jax.vjp(loss_total, weights, images.astype(jnp.float32))
    grads, grad_input = pullback((jnp.ones_like(loss_value), jnp.zeros_like(out_images)))
    new_first = beta_first * first_moment + (1.0 - beta_first) * grads
    new_second = beta_second * second_moment + (1.0 - beta_second) * grads * grads
    fix_first = 1.0 - beta_first ** STEP
    fix_second = 1.0 - beta_second ** STEP
    step_size = new_first / fix_first / (jnp.sqrt(new_second / fix_second) + adam_eps) + weight_decay * master
    new_master = master - learn_rate * step_size
    new_average = ema_keep * average + (1.0 - ema_keep) * new_master
    return (grads, new_first, new_second, new_master, new_average, new_master.astype(jnp.bfloat16), out_images.astype(jnp.bfloat16), grad_input.astype(jnp.bfloat16))
```

```python
import math

import jax
import jax.numpy as jnp
from jax import lax
from jax.experimental import pallas as pl
from jax.experimental.pallas import tpu as pltpu
from jax.sharding import PartitionSpec as P

C = 320
HEADS = 5
HEADSZ = 64
HID = 1280
SIDE = 28
STEP = 3
HALF = 14
NTOK = 784
KEYS = 196


norm_eps = 1e-06
adam_eps = 1e-08
learn_rate = 0.02
weight_decay = 0.05
beta_first = 0.5
beta_second = 0.5
ema_keep = 0.9


def segments():
    return [
        ("norm_gain", (C,)),
        ("norm_bias", (C,)),
        ("query_weight", (C, C)),
        ("query_bias", (C,)),
        ("reduce_weight", (4 * C, C)),
        ("reduce_bias", (C,)),
        ("keys_gain", (C,)),
        ("keys_bias", (C,)),
        ("kv_weight", (C, 2 * C)),
        ("value_bias", (C,)),
        ("out_weight", (C, C)),
        ("out_bias", (C,)),
        ("mlp_gain", (C,)),
        ("mlp_bias", (C,)),
        ("up_weight", (C, HID)),
        ("up_bias", (HID,)),
        ("depth_weight", (9, HID)),
        ("depth_bias", (HID,)),
        ("down_weight", (HID, C)),
        ("down_bias", (C,)),
    ]


def unpack(flat_vector):
    pieces = {}
    offset = 0
    for seg_name, seg_shape in segments():
        seg_size = math.prod(seg_shape)
        pieces[seg_name] = flat_vector[offset : offset + seg_size].reshape(seg_shape)
        offset += seg_size
    return pieces


TOK = 1024
SLAB = 256
KEYC = 208
BLK = 256
NBLK = HID // BLK
F32 = jnp.float32
BF16 = jnp.bfloat16
ERFC_C = 0.35
ERFC_P = (
    0.1397766380054567,
    0.13686603367482672,
    0.1431944963239702,
    0.00881332607675965,
    0.2112475588897874,
    -0.18454519984085327,
    0.04464718332154041,
)
LOG2E = 1.4426950408889634
V_NG, V_NB, V_QB, V_RB, V_KG, V_KB, V_VB, V_OB, V_MG, V_MB, V_DB = range(11)


def dot_nn(left, right):
    return lax.dot_general(left, right, (((1,), (0,)), ((), ())), preferred_element_type=F32)


def dot_nt(left, right):
    return lax.dot_general(left, right, (((1,), (1,)), ((), ())), preferred_element_type=F32)


def fold(x):
    total = x[:, :128]
    for k in range(1, x.shape[1] // 128):
        total = total + x[:, 128 * k : 128 * (k + 1)]
    return total


def aligned(value, step):
    return pl.multiple_of(value, step)


def column(ref, row, lane):
    return ref[pl.ds(row, 8), :][:, lane : lane + 1]


def ln_stats(src, width):
    def first(i, acc):
        return acc + src[pl.ds(aligned(8 * i, 8), 8), :]

    acc = lax.fori_loop(0, C // 8, first, jnp.zeros((8, width), F32), unroll=4)
    mean = jnp.broadcast_to(jnp.sum(acc, 0, keepdims=True) * (1.0 / C), (8, width))

    def second(i, acc):
        d = src[pl.ds(aligned(8 * i, 8), 8), :] - mean
        return acc + d * d

    acc = lax.fori_loop(0, C // 8, second, jnp.zeros((8, width), F32), unroll=4)
    inv = lax.rsqrt(jnp.sum(acc, 0, keepdims=True) * (1.0 / C) + norm_eps)
    return mean, jnp.broadcast_to(inv, (8, width))


def ln_apply(src, dst, mean, inv, vt, gain_lane, bias_lane):
    def step(i, carry):
        row = aligned(16 * i, 16)
        parts = []
        for half in range(2):
            r = aligned(row + 8 * half, 8)
            u = (src[pl.ds(r, 8), :] - mean) * inv
            parts.append(u * column(vt, r, gain_lane) + column(vt, r, bias_lane))
        dst[pl.ds(row, 16), :] = jnp.concatenate(parts, 0).astype(BF16)
        return carry

    lax.fori_loop(0, C // 16, step, 0, unroll=2)


def norm_back(grad, src, mean, inv, vt, gain_lane, gv, gain_slot, bias_slot, emit):
    width = mean.shape[1]

    def first(i, carry):
        acc_one, acc_two = carry
        r = aligned(8 * i, 8)
        u = (src[pl.ds(r, 8), :] - mean) * inv
        d = grad[pl.ds(r, 8), :]
        du = d * u
        gain = column(vt, r, gain_lane)
        gv[gain_slot, pl.ds(r, 8), :] += fold(du)
        gv[bias_slot, pl.ds(r, 8), :] += fold(d)
        return acc_one + d * gain, acc_two + du * gain

    zero = jnp.zeros((8, width), F32)
    acc_one, acc_two = lax.fori_loop(0, C // 8, first, (zero, zero), unroll=2)
    m_one = jnp.broadcast_to(jnp.sum(acc_one, 0, keepdims=True) * (1.0 / C), (8, width))
    m_two = jnp.broadcast_to(jnp.sum(acc_two, 0, keepdims=True) * (1.0 / C), (8, width))

    def second(i, carry):
        row = aligned(16 * i, 16)
        parts = []
        for half in range(2):
            r = aligned(row + 8 * half, 8)
            u = (src[pl.ds(r, 8), :] - mean) * inv
            d = grad[pl.ds(r, 8), :] * column(vt, r, gain_lane)
            parts.append(inv * (d - m_one - u * m_two))
        emit(row, parts)
        return carry

    lax.fori_loop(0, C // 16, second, 0)


def shift_down(v, low):
    a, b = pltpu.roll(v[0], 16, 1), pltpu.roll(v[1], 16, 1)
    return [jnp.where(low, b, a), jnp.where(low, a, b)]


def shift_up(v, high):
    a, b = pltpu.roll(v[0], 112, 1), pltpu.roll(v[1], 112, 1)
    return [jnp.where(high, b, a), jnp.where(high, a, b)]


def side_views(e):
    views = {}
    for a in range(2):
        left = [pltpu.roll(v, 1, 1) for v in e[a, 1]]
        right = [pltpu.roll(v, 127, 1) for v in e[a, 0]]
        views[a, 0] = (left, e[a, 0], e[a, 1])
        views[a, 1] = (e[a, 0], e[a, 1], right)
    return views


def conv(views, taps, bias, low, high):
    def combo(a, b, row):
        out = []
        for h in range(2):
            t = views[a, b][0][h] * taps[row][0]
            t = t + views[a, b][1][h] * taps[row][1]
            out.append(t + views[a, b][2][h] * taps[row][2])
        return out

    result = {}
    for b in range(2):
        top = shift_down(combo(1, b, 0), low)
        mid, bot = combo(0, b, 1), combo(1, b, 2)
        result[0, b] = [top[h] + mid[h] + bot[h] for h in range(2)]
        top, mid = combo(0, b, 0), combo(1, b, 1)
        bot = shift_up(combo(0, b, 2), high)
        result[1, b] = [top[h] + mid[h] + bot[h] for h in range(2)]
        if bias is not None:
            for a in range(2):
                result[a, b] = [v + bias for v in result[a, b]]
    return result


def tap_grads(views, dd, low, high):
    sums = [[None] * 3 for _ in range(3)]
    for b in range(2):
        up = shift_up(dd[0, b], high)
        down = shift_down(dd[1, b], low)
        pairs = ((up, views[1, b], dd[1, b], views[0, b]),
                 (dd[0, b], views[0, b], dd[1, b], views[1, b]),
                 (dd[0, b], views[1, b], down, views[0, b]))
        for row in range(3):
            g_one, v_one, g_two, v_two = pairs[row]
            for col in range(3):
                t = sums[row][col]
                for h in range(2):
                    p = g_one[h] * v_one[col][h] + g_two[h] * v_two[col][h]
                    t = p if t is None else t + p
                sums[row][col] = t
    return sums


def gelu_parts(z):
    t = 1.0 / (1.0 + ERFC_C * jnp.abs(z))
    poly = ERFC_P[6]
    for k in range(5, -1, -1):
        poly = poly * t + ERFC_P[k]
    e = jnp.exp2(z * z * (-0.5 * LOG2E))
    q = poly * t * e
    phi = jnp.where(z < 0, q, 1.0 - q)
    return z * phi, phi + z * e * (1.0 / math.sqrt(2.0 * math.pi))


def image_kernel(
    n_ref, x_ref, ct_ref,
    wqt, wrt, wkvt, wot, wut, wdt, wq, wr, wkv, wo, wu, wd, vt, ht,
    out_ref, gin_ref, gwq_o, gwr_o, gwkv_o, gwo_o, gwu_o, gwd_o, gv_o, gh_o,
    gwq, gwr, gwkv, gwo, gwu, gwd, gv, gh,
    eye, sel, xf, xp, xt, dzt, hgt, qt, att, attb, mt, yt, acc, dgt, dbt, dmt, dqt,
    rt, nt, kvt, kvc, kc, vc, dsb, dkvc, e_s, du_s, u_s, de_s, stat, sem,
):
    slot = pl.program_id(0)
    live = n_ref[0]
    lanes = lax.broadcasted_iota(jnp.int32, (8, 128), 1)
    low, high = lanes < 16, lanes >= 112

    @pl.when(slot == 0)
    def _():
        for ref in (gwq, gwr, gwkv, gwo, gwu, gwd, gv, gh, xp):
            ref[...] = jnp.zeros(ref.shape, ref.dtype)
        r = lax.broadcasted_iota(jnp.int32, (C, C), 0)
        c = lax.broadcasted_iota(jnp.int32, (C, C), 1)
        eye[...] = (r == c).astype(F32).astype(BF16)
        r = lax.broadcasted_iota(jnp.int32, (KEYC, SLAB), 0)
        c = lax.broadcasted_iota(jnp.int32, (KEYC, SLAB), 1)
        i, j = c >> 4, c & 15
        hit = (r == i * HALF + j) & (i < HALF) & (j < HALF)
        sel[...] = hit.astype(F32).astype(BF16)

    def take(src, dst):
        def widen(k, carry):
            row = aligned(112 * k, 16)
            rows = src[0, pl.ds(row, 112), :].astype(F32)
            xf[0, pl.ds(row, 112), :] = rows[:, :128]
            xf[1, pl.ds(row, 112), :] = rows[:, 128:256]
            xf[2, pl.ds(row, 112), :64] = rows[:, 256:]
            return carry

        lax.fori_loop(0, 7, widen, 0)

        def split(i, carry):
            for a in range(2):
                for b in range(2):
                    at = pl.ds(aligned((2 * a + b) * SLAB + 16 * i, 16), HALF)
                    for t in range(3):
                        rows = xf.at[t][pl.ds(56 * i + 28 * a + b, HALF, stride=2), :]
                        xp[at, 128 * t : 128 * (t + 1)] = rows
            return carry

        lax.fori_loop(0, HALF, split, 0)
        for k in range(4):
            part = xp[SLAB * k : SLAB * (k + 1), :C].astype(BF16)
            dst[:, SLAB * k : SLAB * (k + 1)] = dot_nt(eye[...], part).astype(dst.dtype)

    def give(src, dst):
        for k in range(4):
            e_s[:, :C] = dot_nt(eye[:SLAB, :SLAB], src[:, SLAB * k : SLAB * (k + 1)])

            def spread(i, carry):
                at = pl.ds(aligned(16 * i, 16), HALF)
                for t in range(3):
                    rows = e_s[at, 128 * t : 128 * (t + 1)]
                    xf.at[t][pl.ds(56 * i + 28 * (k // 2) + (k % 2), HALF, stride=2), :] = rows
                return carry

            lax.fori_loop(0, HALF, spread, 0)

        def narrow(k, carry):
            row = aligned(112 * k, 16)
            dst[0, pl.ds(row, 112), :128] = xf[0, pl.ds(row, 112), :].astype(BF16)
            dst[0, pl.ds(row, 112), 128:256] = xf[1, pl.ds(row, 112), :].astype(BF16)
            dst[0, pl.ds(row, 112), 256:] = xf[2, pl.ds(row, 112), :64].astype(BF16)
            return carry

        lax.fori_loop(0, 7, narrow, 0)

    @pl.when(slot >= live)
    def _():
        out_ref[...] = jnp.zeros(out_ref.shape, BF16)
        gin_ref[...] = jnp.zeros(gin_ref.shape, BF16)

    @pl.when(slot < live)
    def _():
        take(x_ref, xt)
        take(ct_ref, dzt)
        mean, inv = ln_stats(xt, TOK)
        stat[0], stat[1] = mean, inv
        ln_apply(xt, hgt.at[0], mean, inv, vt, V_NG, V_NB)
        ht_ = hgt.at[0]
        qt[...] = (dot_nn(wqt[...], ht_[...]) + vt[:, V_QB : V_QB + 1]).astype(BF16)
        reduced = vt[:, V_RB : V_RB + 1]
        for k in range(4):
            reduced = reduced + dot_nn(wrt[k], ht_[:, SLAB * k : SLAB * (k + 1)])
        rt[...] = reduced
        kmean, kinv = ln_stats(rt, SLAB)
        stat[4, :, :SLAB], stat[5, :, :SLAB] = kmean, kinv
        ln_apply(rt, nt, kmean, kinv, vt, V_KG, V_KB)
        kvt[:C, :] = dot_nn(wkvt[:C, :], nt[...]).astype(BF16)
        kvt[C:, :] = (dot_nn(wkvt[C:, :], nt[...]) + vt[:, V_VB : V_VB + 1]).astype(BF16)
        kvc[...] = dot_nt(kvt[...], sel[...]).astype(BF16)

        def head_forward(h, carry):
            r = aligned(HEADSZ * h, HEADSZ)
            kc[h] = dot_nt(sel[...], kvt[pl.ds(r, HEADSZ), :]).astype(BF16)
            vc[h] = dot_nt(sel[...], kvt[pl.ds(aligned(C + r, HEADSZ), HEADSZ), :]).astype(BF16)
            att[h] = dot_nn(kc[h], qt[pl.ds(r, HEADSZ), :])

            def tile(t, carry):
                ls = pl.ds(aligned(128 * t, 128), 128)
                s = att[h, :, ls]
                rows = lax.broadcasted_iota(jnp.int32, (KEYC, 128), 0)
                s = jnp.where(rows < KEYS, s, -jnp.inf)
                top = jnp.max(s, 0, keepdims=True)
                p = jnp.exp2((s - top) * (LOG2E * HEADSZ**-0.5))
                p = p * (1.0 / jnp.sum(p, 0, keepdims=True))
                att[h, :, ls] = p
                attb[h, :, ls] = p.astype(BF16)
                return carry

            lax.fori_loop(0, TOK // 128, tile, 0)
            vt_h = kvc[pl.ds(aligned(C + r, HEADSZ), HEADSZ), :]
            mt[pl.ds(r, HEADSZ), :] = dot_nn(vt_h, attb[h]).astype(BF16)
            return carry

        lax.fori_loop(0, HEADS, head_forward, 0)
        yt[...] = xt[...] + (dot_nn(wot[...], mt[...]) + vt[:, V_OB : V_OB + 1])
        mean, inv = ln_stats(yt, TOK)
        stat[2], stat[3] = mean, inv
        ln_apply(yt, hgt.at[1], mean, inv, vt, V_MG, V_MB)
        gt = hgt.at[1]
        acc[...] = yt[...] + vt[:, V_DB : V_DB + 1]
        dgt[...] = jnp.zeros(dgt.shape, F32)
        lane16 = (lanes & 15) < HALF
        keep = (lane16, lane16 & (lanes < 96))

        def block(c, carry):
            e_s[...] = dot_nn(wut[c], gt[...])
            du_s[...] = dot_nn(wd[c], dzt[...])

            def group(i, carry):
                row = aligned(16 * i, 16)
                u_parts, de_parts = [], []
                for half in range(2):
                    r = aligned(row + 8 * half, 8)
                    chan = aligned(BLK * c + r, 8)
                    table = ht[pl.ds(chan, 8), :]
                    w = [jnp.broadcast_to(table[:, k : k + 1], (8, 128)) for k in range(11)]
                    taps = [w[0:3], w[3:6], w[6:9]]
                    flipped = [[w[8], w[7], w[6]], [w[5], w[4], w[3]], [w[2], w[1], w[0]]]
                    e = {}
                    for k in range(4):
                        e[k // 2, k % 2] = [
                            jnp.where(
                                keep[q],
                                e_s[pl.ds(r, 8), SLAB * k + 128 * q : SLAB * k + 128 * (q + 1)] + w[9],
                                0.0,
                            )
                            for q in range(2)
                        ]
                    views = side_views(e)
                    d = conv(views, taps, w[10], low, high)
                    dd, us = {}, []
                    for k in range(4):
                        out = []
                        for q in range(2):
                            value, slope = gelu_parts(d[k // 2, k % 2][q])
                            us.append(value)
                            out.append(
                                du_s[pl.ds(r, 8), SLAB * k + 128 * q : SLAB * k + 128 * (q + 1)] * slope
                            )
                        dd[k // 2, k % 2] = out
                    u_parts.append(us)
                    gsum = None
                    for k in range(4):
                        for q in range(2):
                            v = dd[k // 2, k % 2][q]
                            gsum = v if gsum is None else gsum + v
                    gh[10, pl.ds(chan, 8), :] += gsum
                    sums = tap_grads(views, dd, low, high)
                    for k in range(9):
                        gh[k, pl.ds(chan, 8), :] += sums[k // 3][k % 3]
                    de = conv(side_views(dd), flipped, None, low, high)
                    des = [
                        jnp.where(keep[q], de[k // 2, k % 2][q], 0.0) for k in range(4) for q in range(2)
                    ]
                    de_parts.append(des)
                esums = [None, None]
                for k in range(8):
                    ls = slice(128 * k, 128 * (k + 1))
                    u_s[pl.ds(row, 16), ls] = jnp.concatenate(
                        [u_parts[0][k], u_parts[1][k]], 0
                    ).astype(BF16)
                    de16 = jnp.concatenate([de_parts[0][k], de_parts[1][k]], 0).astype(BF16)
                    de_s[pl.ds(row, 16), ls] = de16
                    wide = de16.astype(F32)
                    for half in range(2):
                        v = wide[8 * half : 8 * half + 8]
                        esums[half] = v if esums[half] is None else esums[half] + v
                chan = aligned(BLK * c + row, 16)
                gh[9, pl.ds(chan, 8), :] += esums[0]
                gh[9, pl.ds(aligned(chan + 8, 8), 8), :] += esums[1]
                return carry

            lax.fori_loop(0, BLK // 16, group, 0)
            acc[...] += dot_nn(wdt[c], u_s[...])
            dgt[...] += dot_nn(wu[c], de_s[...])
            gwd[c] += dot_nt(u_s[...], dzt[...])
            gwu[c] += dot_nt(gt[...], de_s[...])
            return carry

        lax.fori_loop(0, NBLK, block, 0)
        dbt[...] = acc[...].astype(BF16)
        give(dbt, out_ref)

        def middle(row, parts):
            for half in range(2):
                r = aligned(row + 8 * half, 8)
                z = dzt[pl.ds(row, 16), :].astype(F32)[8 * half : 8 * half + 8]
                gv[V_DB, pl.ds(r, 8), :] += fold(z)
                parts[half] = parts[half] + z
            both = jnp.concatenate(parts, 0)
            acc[pl.ds(row, 16), :] = both
            low_part = both.astype(BF16)
            dbt[pl.ds(row, 16), :] = low_part
            wide = low_part.astype(F32)
            for half in range(2):
                r = aligned(row + 8 * half, 8)
                gv[V_OB, pl.ds(r, 8), :] += fold(wide[8 * half : 8 * half + 8])

        norm_back(dgt, yt, stat[2], stat[3], vt, V_MG, gv, V_MG, V_MB, middle)
        dmt[...] = dot_nn(wo[...], dbt[...]).astype(BF16)
        gwo[...] += dot_nt(mt[...], dbt[...])

        def head_backward(h, carry):
            r = aligned(HEADSZ * h, HEADSZ)
            hs = pl.ds(r, HEADSZ)
            da = e_s.at[pl.ds(0, KEYC), :]
            da[...] = dot_nn(vc[h], dmt[hs, :])

            def tile(t, carry):
                ls = pl.ds(aligned(128 * t, 128), 128)
                p = att[h, :, ls]
                g = da[:, ls]
                total = jnp.sum(p * g, 0, keepdims=True)
                dsb[:, ls] = (p * (g - total)).astype(BF16)
                return carry

            lax.fori_loop(0, TOK // 128, tile, 0)
            dkvc[pl.ds(aligned(C + r, HEADSZ), HEADSZ), :] = dot_nt(dmt[hs, :], attb[h]).astype(BF16)
            dqt[hs, :] = (dot_nn(kvc[hs, :], dsb[...]) * HEADSZ**-0.5).astype(BF16)
            dkvc[hs, :] = (dot_nt(qt[hs, :], dsb[...]) * HEADSZ**-0.5).astype(BF16)
            return carry

        lax.fori_loop(0, HEADS, head_backward, 0)
        kvt[...] = dot_nn(dkvc[...], sel[...]).astype(BF16)
        gwkv[...] += dot_nt(nt[...], kvt[...])
        dnt = dgt.at[:, pl.ds(0, SLAB)]
        dnt[...] = dot_nn(wkv[...], kvt[...])

        def vbias(i, carry):
            row = aligned(16 * i, 16)
            wide = kvt[pl.ds(aligned(C + row, 16), 16), :].astype(F32)
            gv[V_VB, pl.ds(row, 16), :] += fold(wide)
            return carry

        lax.fori_loop(0, C // 16, vbias, 0)

        def keys_out(row, parts):
            low_part = jnp.concatenate(parts, 0).astype(BF16)
            nt[pl.ds(row, 16), :] = low_part
            gv[V_RB, pl.ds(row, 16), :] += fold(low_part.astype(F32))

        norm_back(
            dnt, rt, stat[4, :, :SLAB], stat[5, :, :SLAB], vt, V_KG, gv, V_KG, V_KB, keys_out
        )
        for k in range(4):
            ls = slice(SLAB * k, SLAB * (k + 1))
            gwr[k] += dot_nt(ht_[:, ls], nt[...])
            dgt[:, ls] = dot_nn(wq[...], dqt[:, ls]) + dot_nn(wr[k], nt[...])
        gwq[...] += dot_nt(ht_[...], dqt[...])

        def qbias(i, carry):
            row = aligned(16 * i, 16)
            gv[V_QB, pl.ds(row, 16), :] += fold(dqt[pl.ds(row, 16), :].astype(F32))
            return carry

        lax.fori_loop(0, C // 16, qbias, 0)

        def final(row, parts):
            both = jnp.concatenate(parts, 0) + acc[pl.ds(row, 16), :]
            dbt[pl.ds(row, 16), :] = both.astype(BF16)

        norm_back(dgt, xt, stat[0], stat[1], vt, V_NG, gv, V_NG, V_NB, final)
        give(dbt, gin_ref)

    @pl.when(slot == pl.num_programs(0) - 1)
    def _():
        pairs = (
            (gwq, gwq_o), (gwr, gwr_o), (gwkv, gwkv_o), (gwo, gwo_o),
            (gwu, gwu_o), (gwd, gwd_o), (gv, gv_o), (gh, gh_o),
        )
        copies = [pltpu.make_async_copy(a, b, sem.at[k]) for k, (a, b) in enumerate(pairs)]
        for cp in copies:
            cp.start()
        for cp in copies:
            cp.wait()


def run_images(live, images, cotangent, weights):
    slots = images.shape[0]
    item = pl.BlockSpec((1, NTOK, C), lambda s, n: (jnp.minimum(s, n[0] - 1), 0, 0))
    out_item = pl.BlockSpec((1, NTOK, C), lambda s, n: (s, 0, 0))

    def fixed(array):
        dims = array.shape
        return pl.BlockSpec(dims, lambda s, n: (0,) * len(dims), pipeline_mode=pl.Buffered(1))

    anywhere = pl.BlockSpec(memory_space=pl.ANY)
    grads = [
        (C, C), (4, C, C), (C, 2 * C), (C, C), (NBLK, C, BLK), (NBLK, BLK, C),
        (11, C, 128), (11, HID, 128),
    ]
    wide = lambda *dims: pltpu.VMEM(dims, F32)
    thin = lambda *dims: pltpu.VMEM(dims, BF16)
    scratch = [wide(*dims) for dims in grads] + [
        thin(C, C), thin(KEYC, SLAB), wide(3, NTOK, 128), wide(TOK, 384),
        wide(C, TOK), thin(C, TOK), thin(2, C, TOK), thin(C, TOK),
        wide(HEADS, KEYC, TOK), thin(HEADS, KEYC, TOK), thin(C, TOK), wide(C, TOK),
        wide(C, TOK), wide(C, TOK), thin(C, TOK), thin(C, TOK), thin(C, TOK),
        wide(C, SLAB), thin(C, SLAB), thin(2 * C, SLAB), thin(2 * C, KEYC),
        thin(HEADS, KEYC, HEADSZ), thin(HEADS, KEYC, HEADSZ), thin(KEYC, TOK), thin(2 * C, KEYC),
        wide(BLK, TOK), wide(BLK, TOK), thin(BLK, TOK), thin(BLK, TOK), wide(6, 8, TOK),
        pltpu.SemaphoreType.DMA((len(grads),)),
    ]
    call = pl.pallas_call(
        image_kernel,
        out_shape=[jax.ShapeDtypeStruct(images.shape, BF16)] * 2
        + [jax.ShapeDtypeStruct(dims, F32) for dims in grads],
        grid_spec=pltpu.PrefetchScalarGridSpec(
            num_scalar_prefetch=1,
            grid=(slots,),
            in_specs=[item, item] + [fixed(w) for w in weights],
            out_specs=[out_item, out_item] + [anywhere] * len(grads),
            scratch_shapes=scratch,
        ),
        compiler_params=pltpu.CompilerParams(
            dimension_semantics=("arbitrary",), vmem_limit_bytes=67043328
        ),
        name="image_block",
    )
    return call(live, images, cotangent, *weights)


def prepare(p):
    wq, wo, wkv = p["query_weight"], p["out_weight"], p["kv_weight"]
    wr = p["reduce_weight"].reshape(4, C, C)
    wu = p["up_weight"].reshape(C, NBLK, BLK).transpose(1, 0, 2)
    wd = p["down_weight"].reshape(NBLK, BLK, C)
    flip = lambda w: jnp.swapaxes(w, -1, -2)
    names = (
        "norm_gain", "norm_bias", "query_bias", "reduce_bias", "keys_gain", "keys_bias",
        "value_bias", "out_bias", "mlp_gain", "mlp_bias", "down_bias",
    )
    vt = jnp.stack([p[n] for n in names], 1).astype(F32)
    ht = jnp.concatenate([p["depth_weight"], p["up_bias"][None], p["depth_bias"][None]], 0).T
    vt = jnp.pad(vt, ((0, 0), (0, 128 - 11)))
    ht = jnp.pad(ht.astype(F32), ((0, 0), (0, 128 - 11)))
    return [
        flip(wq), flip(wr), flip(wkv), flip(wo), flip(wu), flip(wd),
        wq, wr, wkv, wo, wu, wd, vt, ht,
    ]


def collect(gwq, gwr, gwkv, gwo, gwu, gwd, gv, gh):
    v = jnp.sum(gv, -1)
    h = jnp.sum(gh, -1)
    return {
        "norm_gain": v[V_NG], "norm_bias": v[V_NB], "query_weight": gwq, "query_bias": v[V_QB],
        "reduce_weight": gwr, "reduce_bias": v[V_RB], "keys_gain": v[V_KG], "keys_bias": v[V_KB],
        "kv_weight": gwkv, "value_bias": v[V_VB], "out_weight": gwo, "out_bias": v[V_OB],
        "mlp_gain": v[V_MG], "mlp_bias": v[V_MB], "up_weight": gwu.transpose(1, 0, 2),
        "up_bias": h[9], "depth_weight": h[:9], "depth_bias": h[10], "down_weight": gwd,
        "down_bias": v[V_DB],
    }


def body(images, counts, cotangent, master, first_moment, second_moment, average):
    shard_low = master.astype(jnp.bfloat16)
    pieces = unpack(lax.all_gather(shard_low, ("dp", "fsdp"), axis=0, tiled=True))
    results = run_images(counts, images, cotangent, prepare(pieces))
    output_images, grad_images = results[:2]
    terms = collect(*results[2:])
    flat_grads = jnp.concatenate([terms[n].reshape(-1) for n, _ in segments()])
    full_length = master.shape[0] * lax.axis_size("dp") * lax.axis_size("fsdp")
    flat_grads = jnp.pad(flat_grads, (0, full_length - flat_grads.shape[0]))
    grads = lax.psum_scatter(flat_grads, ("dp", "fsdp"), scatter_dimension=0, tiled=True)
    new_first = beta_first * first_moment + (1.0 - beta_first) * grads
    new_second = beta_second * second_moment + (1.0 - beta_second) * grads * grads
    fix_first = 1.0 - beta_first**STEP
    fix_second = 1.0 - beta_second**STEP
    step_size = (
        new_first / fix_first / (jnp.sqrt(new_second / fix_second) + adam_eps)
        + weight_decay * master
    )
    new_master = master - learn_rate * step_size
    new_average = ema_keep * average + (1.0 - ema_keep) * new_master
    return (
        grads,
        new_first,
        new_second,
        new_master,
        new_average,
        new_master.astype(jnp.bfloat16),
        output_images,
        grad_images,
    )


def solution(mesh):
    return jax.shard_map(
        body,
        mesh=mesh,
        in_specs=(
            P(("dp", "fsdp"), None, None),
            P(("dp", "fsdp")),
            P(("dp", "fsdp"), None, None),
            P(("dp", "fsdp")),
            P(("dp", "fsdp")),
            P(("dp", "fsdp")),
            P(("dp", "fsdp")),
        ),
        out_specs=(
            P(("dp", "fsdp")),
            P(("dp", "fsdp")),
            P(("dp", "fsdp")),
            P(("dp", "fsdp")),
            P(("dp", "fsdp")),
            P(("dp", "fsdp")),
            P(("dp", "fsdp"), None, None),
            P(("dp", "fsdp"), None, None),
        ),
        check_vma=False,
    )
```

```python
import functools
import math

import jax
import jax.numpy as jnp
from jax import lax
from jax.experimental import pallas as pl
from jax.experimental.pallas import tpu as pltpu
from jax.sharding import PartitionSpec as P

C = 320
HEADS = 5
HEADSZ = 64
HID = 1280
SIDE = 28
STEP = 3
HALF = 14
NTOK = 784
KEYS = 196


norm_eps = 1e-06
adam_eps = 1e-08
learn_rate = 0.02
weight_decay = 0.05
beta_first = 0.5
beta_second = 0.5
ema_keep = 0.9


TOK = 1024
SLAB = 256
KEYC = 208
BLK = 256
NBLK = HID // BLK
F32 = jnp.float32
BF16 = jnp.bfloat16
ERFC_C = 0.35
ERFC_P = (
    0.1397766380054567,
    0.13686603367482672,
    0.1431944963239702,
    0.00881332607675965,
    0.2112475588897874,
    -0.18454519984085327,
    0.04464718332154041,
)
LOG2E = 1.4426950408889634
V_NG, V_NB, V_QB, V_RB, V_KG, V_KB, V_VB, V_OB, V_MG, V_MB, V_DB = range(11)


def dot_nn(left, right):
    return lax.dot_general(left, right, (((1,), (0,)), ((), ())), preferred_element_type=F32)


def dot_nt(left, right):
    return lax.dot_general(left, right, (((1,), (1,)), ((), ())), preferred_element_type=F32)


def fold(x):
    total = x[:, :128]
    for k in range(1, x.shape[1] // 128):
        total = total + x[:, 128 * k : 128 * (k + 1)]
    return total


def aligned(value, step):
    return pl.multiple_of(value, step)


def column(ref, row, lane):
    return ref[pl.ds(row, 8), :][:, lane : lane + 1]


def ln_stats(src, width):
    def first(i, acc):
        return acc + src[pl.ds(aligned(8 * i, 8), 8), :]

    acc = lax.fori_loop(0, C // 8, first, jnp.zeros((8, width), F32), unroll=4)
    mean = jnp.broadcast_to(jnp.sum(acc, 0, keepdims=True) * (1.0 / C), (8, width))

    def second(i, acc):
        d = src[pl.ds(aligned(8 * i, 8), 8), :] - mean
        return acc + d * d

    acc = lax.fori_loop(0, C // 8, second, jnp.zeros((8, width), F32), unroll=4)
    inv = lax.rsqrt(jnp.sum(acc, 0, keepdims=True) * (1.0 / C) + norm_eps)
    return mean, jnp.broadcast_to(inv, (8, width))


def ln_apply(src, dst, mean, inv, vt, gain_lane, bias_lane):
    def step(i, carry):
        row = aligned(16 * i, 16)
        parts = []
        for half in range(2):
            r = aligned(row + 8 * half, 8)
            u = (src[pl.ds(r, 8), :] - mean) * inv
            parts.append(u * column(vt, r, gain_lane) + column(vt, r, bias_lane))
        dst[pl.ds(row, 16), :] = jnp.concatenate(parts, 0).astype(BF16)
        return carry

    lax.fori_loop(0, C // 16, step, 0, unroll=2)


def norm_back(grad, src, mean, inv, vt, gain_lane, gv, gain_slot, bias_slot, emit):
    width = mean.shape[1]

    def first(i, carry):
        acc_one, acc_two = carry
        r = aligned(8 * i, 8)
        u = (src[pl.ds(r, 8), :] - mean) * inv
        d = grad[pl.ds(r, 8), :]
        du = d * u
        gain = column(vt, r, gain_lane)
        gv[gain_slot, pl.ds(r, 8), :] += fold(du)
        gv[bias_slot, pl.ds(r, 8), :] += fold(d)
        return acc_one + d * gain, acc_two + du * gain

    zero = jnp.zeros((8, width), F32)
    acc_one, acc_two = lax.fori_loop(0, C // 8, first, (zero, zero), unroll=2)
    m_one = jnp.broadcast_to(jnp.sum(acc_one, 0, keepdims=True) * (1.0 / C), (8, width))
    m_two = jnp.broadcast_to(jnp.sum(acc_two, 0, keepdims=True) * (1.0 / C), (8, width))

    def second(i, carry):
        row = aligned(16 * i, 16)
        parts = []
        for half in range(2):
            r = aligned(row + 8 * half, 8)
            u = (src[pl.ds(r, 8), :] - mean) * inv
            d = grad[pl.ds(r, 8), :] * column(vt, r, gain_lane)
            parts.append(inv * (d - m_one - u * m_two))
        emit(row, parts)
        return carry

    lax.fori_loop(0, C // 16, second, 0)


def shift_down(v, low):
    a, b = pltpu.roll(v[0], 16, 1), pltpu.roll(v[1], 16, 1)
    return [jnp.where(low, b, a), jnp.where(low, a, b)]


def shift_up(v, high):
    a, b = pltpu.roll(v[0], 112, 1), pltpu.roll(v[1], 112, 1)
    return [jnp.where(high, b, a), jnp.where(high, a, b)]


def side_views(e):
    views = {}
    for a in range(2):
        left = [pltpu.roll(v, 1, 1) for v in e[a, 1]]
        right = [pltpu.roll(v, 127, 1) for v in e[a, 0]]
        views[a, 0] = (left, e[a, 0], e[a, 1])
        views[a, 1] = (e[a, 0], e[a, 1], right)
    return views


def conv(views, taps, bias, low, high):
    def combo(a, b, row):
        out = []
        for h in range(2):
            t = views[a, b][0][h] * taps[row][0]
            t = t + views[a, b][1][h] * taps[row][1]
            out.append(t + views[a, b][2][h] * taps[row][2])
        return out

    result = {}
    for b in range(2):
        top = shift_down(combo(1, b, 0), low)
        mid, bot = combo(0, b, 1), combo(1, b, 2)
        result[0, b] = [top[h] + mid[h] + bot[h] for h in range(2)]
        top, mid = combo(0, b, 0), combo(1, b, 1)
        bot = shift_up(combo(0, b, 2), high)
        result[1, b] = [top[h] + mid[h] + bot[h] for h in range(2)]
        if bias is not None:
            for a in range(2):
                result[a, b] = [v + bias for v in result[a, b]]
    return result


def tap_grads(views, dd, low, high):
    sums = [[None] * 3 for _ in range(3)]
    for b in range(2):
        up = shift_up(dd[0, b], high)
        down = shift_down(dd[1, b], low)
        pairs = ((up, views[1, b], dd[1, b], views[0, b]),
                 (dd[0, b], views[0, b], dd[1, b], views[1, b]),
                 (dd[0, b], views[1, b], down, views[0, b]))
        for row in range(3):
            g_one, v_one, g_two, v_two = pairs[row]
            for col in range(3):
                t = sums[row][col]
                for h in range(2):
                    p = g_one[h] * v_one[col][h] + g_two[h] * v_two[col][h]
                    t = p if t is None else t + p
                sums[row][col] = t
    return sums


def gelu_parts(z):
    t = 1.0 / (1.0 + ERFC_C * jnp.abs(z))
    poly = ERFC_P[6]
    for k in range(5, -1, -1):
        poly = poly * t + ERFC_P[k]
    e = jnp.exp2(z * z * (-0.5 * LOG2E))
    q = poly * t * e
    phi = jnp.where(z < 0, q, 1.0 - q)
    return z * phi, phi + z * e * (1.0 / math.sqrt(2.0 * math.pi))


ROW_QUERY, ROW_REDUCE, ROW_KEYS, ROW_KV = 0, 805, 4010, 4015
ROW_VALUE, ROW_UP, ROW_HID, ROW_DOWN = 5615, 6425, 9625, 9735


def rows_from_flat(flat, base, pairs, buf):
    left = lax.broadcasted_iota(jnp.int32, (8, 128), 1) < 64

    def step(i, carry):
        t = [flat[pl.ds(base + 40 * i + k, 8, stride=5), :] for k in range(5)]
        r = [pltpu.roll(t[k], 64, 1) for k in range(2, 5)]
        even = (t[0], t[1], t[2])
        odd = (jnp.where(left, r[0], r[1]), jnp.where(left, r[1], r[2]), r[2])
        for k in range(3):
            buf.at[k][pl.ds(16 * i, 8, stride=2), :] = even[k]
            buf.at[k][pl.ds(16 * i + 1, 8, stride=2), :] = odd[k]
        return carry

    lax.fori_loop(0, -(-pairs // 8), step, 0)


def rows_to_flat(flat, base, pairs, buf):
    left = lax.broadcasted_iota(jnp.int32, (8, 128), 1) < 64

    def emit(i, size):
        even = [buf.at[k][pl.ds(16 * i, size, stride=2), :] for k in range(3)]
        odd = [buf.at[k][pl.ds(16 * i + 1, size, stride=2), :] for k in range(3)]
        r = [pltpu.roll(odd[k], 64, 1) for k in range(3)]
        lo = left[:size]
        t = (even[0], even[1], jnp.where(lo, even[2], r[0]),
             jnp.where(lo, r[0], r[1]), jnp.where(lo, r[1], r[2]))
        for k in range(5):
            flat[pl.ds(base + 40 * i + k, size, stride=5), :] = t[k]

    def step(i, carry):
        emit(i, 8)
        return carry

    lax.fori_loop(0, pairs // 8, step, 0)
    if pairs % 8:
        emit(pairs // 8, pairs % 8)


def buf_rows(buf, start, size):
    at = slice(start, start + size)
    return jnp.concatenate([buf[0, at], buf[1, at], buf[2, at][:, :64]], 1)


def put_rows(buf, start, value):
    at = slice(start, start + value.shape[0])
    buf[0, at] = value[:, :128]
    buf[1, at] = value[:, 128:256]
    buf[2, at, :64] = value[:, 256:]


def unpack_weights(
    shard_rows, wall, flat, buf, eye,
    wqt, wrt, wkvt, wot, wut, wdt, wq, wr, wkv, wo, wu, wd, vt, ht,
):
    for k in range(wall.shape[0]):
        flat[shard_rows * k : shard_rows * (k + 1), :] = wall[k, :shard_rows].astype(F32)
    tail = shard_rows * wall.shape[0]
    flat[tail:, :] = jnp.zeros((flat.shape[0] - tail, 128), F32)
    vectors = {}

    def vector(slot, row):
        vectors[slot] = [buf[t, row : row + 1, :] for t in range(3)]

    def flip(w):
        return dot_nt(eye[: w.shape[1], : w.shape[1]], w).astype(BF16)

    rows_from_flat(flat, ROW_QUERY, 161, buf)
    wq[...] = buf_rows(buf, 2, C).astype(BF16)
    vector(V_NG, 0)
    vector(V_NB, 1)
    wqt[...] = flip(wq[...])
    rows_from_flat(flat, ROW_REDUCE, 641, buf)
    for k in range(4):
        wr[k] = buf_rows(buf, 1 + C * k, C).astype(BF16)
        wrt[k] = flip(wr[k])
    vector(V_QB, 0)
    vector(V_RB, 1281)
    rows_from_flat(flat, ROW_KEYS, 1, buf)
    vector(V_KG, 0)
    vector(V_KB, 1)
    for k in range(5):
        cols = flat[pl.ds(ROW_KV + k, C, stride=5), :]
        wkv[:, 128 * k : 128 * (k + 1)] = cols.astype(BF16)
        wkvt[128 * k : 128 * (k + 1), :] = flip(wkv[:, 128 * k : 128 * (k + 1)])
    rows_from_flat(flat, ROW_VALUE, 162, buf)
    wo[...] = buf_rows(buf, 1, C).astype(BF16)
    wot[...] = flip(wo[...])
    vector(V_VB, 0)
    vector(V_OB, 321)
    vector(V_MG, 322)
    vector(V_MB, 323)
    for k in range(10):
        cols = flat[pl.ds(ROW_UP + k, C, stride=10), :]
        wu[:, 128 * k : 128 * (k + 1)] = cols.astype(BF16)
        wut[128 * k : 128 * (k + 1), :] = flip(wu[:, 128 * k : 128 * (k + 1)])
    rows_from_flat(flat, ROW_DOWN, 641, buf)
    for k in range(5):
        at = slice(BLK * k, BLK * (k + 1))
        wd[at, :] = buf_rows(buf, BLK * k, BLK).astype(BF16)
        wdt[:, at] = flip(wd[at, :])
    vector(V_DB, 1280)
    for t in range(3):
        rows = jnp.concatenate([vectors[k][t] for k in range(11)] + [jnp.zeros((117, 128), F32)], 0)
        size = min(128, C - 128 * t)
        vt[128 * t : 128 * t + size, :] = rows.T[:size]
    for k in range(10):
        rows = flat[pl.ds(ROW_HID + k, 11, stride=10), :]
        rows = jnp.concatenate([rows, jnp.zeros((117, 128), F32)], 0)
        ht[128 * k : 128 * (k + 1), :] = rows.T


def pack_grads(shard_rows, flat, buf, gwq, gwr, gwkv, gwo, gwu, gwd, gv, gh):
    flat[ROW_DOWN + 3200 :, :] = jnp.zeros((flat.shape[0] - ROW_DOWN - 3200, 128), F32)

    def vector(slot, row):
        for t in range(3):
            size = min(128, C - 128 * t)
            part = gv[slot, 128 * t : 128 * t + size, :]
            if size < 128:
                part = jnp.concatenate([part, jnp.zeros((128 - size, 128), F32)], 0)
            buf[t, row : row + 1, :] = jnp.sum(part.T, 0, keepdims=True)

    put_rows(buf, 2, gwq[...])
    vector(V_NG, 0)
    vector(V_NB, 1)
    rows_to_flat(flat, ROW_QUERY, 161, buf)
    for k in range(4):
        put_rows(buf, 1 + C * k, gwr[k])
    vector(V_QB, 0)
    vector(V_RB, 1281)
    rows_to_flat(flat, ROW_REDUCE, 641, buf)
    vector(V_KG, 0)
    vector(V_KB, 1)
    rows_to_flat(flat, ROW_KEYS, 1, buf)
    for k in range(5):
        flat[pl.ds(ROW_KV + k, C, stride=5), :] = gwkv[:, 128 * k : 128 * (k + 1)]
    put_rows(buf, 1, gwo[...])
    vector(V_VB, 0)
    vector(V_OB, 321)
    vector(V_MG, 322)
    vector(V_MB, 323)
    rows_to_flat(flat, ROW_VALUE, 162, buf)
    for k in range(10):
        flat[pl.ds(ROW_UP + k, C, stride=10), :] = gwu[:, 128 * k : 128 * (k + 1)]
        for slot in range(11):
            part = gh[slot, 128 * k : 128 * (k + 1), :]
            at = ROW_HID + 10 * slot + k
            flat[at : at + 1, :] = jnp.sum(part.T, 0, keepdims=True)
    put_rows(buf, 0, gwd[...])
    vector(V_DB, 1280)
    for t in range(3):
        buf[t, 1281:1282, :] = jnp.zeros((1, 128), F32)
    rows_to_flat(flat, ROW_DOWN, 641, buf)
    half = ROW_DOWN + 3202
    flat[half : half + 1, 64:] = jnp.zeros((1, 64), F32)
    flat[half + 1 :, :] = jnp.zeros((flat.shape[0] - half - 1, 128), F32)


def image_kernel(
    shard_rows, n_ref, x_ref, ct_ref, wall,
    out_ref, gin_ref, gflat,
    wqt, wrt, wkvt, wot, wut, wdt, wq, wr, wkv, wo, wu, wd, vt, ht,
    gwq, gwr, gwkv, gwo, gwu, gwd, gv, gh,
    eye, sel, flat, xf, xp, xt, dzt, hgt, qt, attb, mt, yt, acc, dgt, dbt, dmt, dqt,
    rt, nt, kvt, kvc, kc, vc, dsb, dkvc, e_s, du_s, u_s, de_s, stat, stage, sem,
):
    slot = pl.program_id(0)
    live = n_ref[0]
    lanes = lax.broadcasted_iota(jnp.int32, (8, 128), 1)
    low, high = lanes < 16, lanes >= 112

    @pl.when(slot == 0)
    def _():
        for ref in (gwq, gwr, gwkv, gwo, gwu, gwd, gv, gh):
            ref[...] = jnp.zeros(ref.shape, ref.dtype)
        r = lax.broadcasted_iota(jnp.int32, (C, C), 0)
        c = lax.broadcasted_iota(jnp.int32, (C, C), 1)
        eye[...] = (r == c).astype(F32).astype(BF16)
        r = lax.broadcasted_iota(jnp.int32, (KEYC, SLAB), 0)
        c = lax.broadcasted_iota(jnp.int32, (KEYC, SLAB), 1)
        i, j = c >> 4, c & 15
        hit = (r == i * HALF + j) & (i < HALF) & (j < HALF)
        sel[...] = hit.astype(F32).astype(BF16)
        unpack_weights(
            shard_rows, wall, flat, xp, eye,
            wqt, wrt, wkvt, wot, wut, wdt, wq, wr, wkv, wo, wu, wd, vt, ht,
        )
        xp[...] = jnp.zeros(xp.shape, F32)

    def take(src, dst):
        def widen(k, carry):
            row = aligned(112 * k, 16)
            rows = src[0, pl.ds(row, 112), :].astype(F32)
            xf[0, pl.ds(row, 112), :] = rows[:, :128]
            xf[1, pl.ds(row, 112), :] = rows[:, 128:256]
            xf[2, pl.ds(row, 112), :64] = rows[:, 256:]
            return carry

        lax.fori_loop(0, 7, widen, 0)

        def split(i, carry):
            for a in range(2):
                for b in range(2):
                    at = pl.ds(aligned((2 * a + b) * SLAB + 16 * i, 16), HALF)
                    for t in range(3):
                        rows = xf.at[t][pl.ds(56 * i + 28 * a + b, HALF, stride=2), :]
                        xp[t, at, :] = rows
            return carry

        lax.fori_loop(0, HALF, split, 0)
        for k in range(4):
            ks = slice(SLAB * k, SLAB * (k + 1))
            part = jnp.concatenate([xp[0, ks], xp[1, ks], xp[2, ks][:, :64]], 1).astype(BF16)
            dst[:, SLAB * k : SLAB * (k + 1)] = dot_nt(eye[...], part).astype(dst.dtype)

    def give(src, dst):
        for k in range(4):
            e_s[:, :C] = dot_nt(eye[:SLAB, :SLAB], src[:, SLAB * k : SLAB * (k + 1)])

            def spread(i, carry):
                at = pl.ds(aligned(16 * i, 16), HALF)
                for t in range(3):
                    rows = e_s[at, 128 * t : 128 * (t + 1)]
                    xf.at[t][pl.ds(56 * i + 28 * (k // 2) + (k % 2), HALF, stride=2), :] = rows
                return carry

            lax.fori_loop(0, HALF, spread, 0)

        def narrow(k, carry):
            row = aligned(112 * k, 16)
            dst[0, pl.ds(row, 112), :128] = xf[0, pl.ds(row, 112), :].astype(BF16)
            dst[0, pl.ds(row, 112), 128:256] = xf[1, pl.ds(row, 112), :].astype(BF16)
            dst[0, pl.ds(row, 112), 256:] = xf[2, pl.ds(row, 112), :64].astype(BF16)
            return carry

        lax.fori_loop(0, 7, narrow, 0)

    @pl.when(slot >= live)
    def _():
        out_ref[...] = jnp.zeros(out_ref.shape, BF16)
        gin_ref[...] = jnp.zeros(gin_ref.shape, BF16)

    @pl.when(slot < live)
    def _():
        take(x_ref, xt)
        take(ct_ref, dzt)
        mean, inv = ln_stats(xt, TOK)
        stat[0], stat[1] = mean, inv
        ln_apply(xt, hgt.at[0], mean, inv, vt, V_NG, V_NB)
        ht_ = hgt.at[0]
        qt[...] = (dot_nn(wqt[...], ht_[...]) + vt[:, V_QB : V_QB + 1]).astype(BF16)
        reduced = vt[:, V_RB : V_RB + 1]
        for k in range(4):
            reduced = reduced + dot_nn(wrt[k], ht_[:, SLAB * k : SLAB * (k + 1)])
        rt[...] = reduced
        kmean, kinv = ln_stats(rt, SLAB)
        stat[4, :, :SLAB], stat[5, :, :SLAB] = kmean, kinv
        ln_apply(rt, nt, kmean, kinv, vt, V_KG, V_KB)
        kvt[:C, :] = dot_nn(wkvt[:C, :], nt[...]).astype(BF16)
        kvt[C:, :] = (dot_nn(wkvt[C:, :], nt[...]) + vt[:, V_VB : V_VB + 1]).astype(BF16)
        kvc[...] = dot_nt(kvt[...], sel[...]).astype(BF16)

        def head_forward(h, carry):
            r = aligned(HEADSZ * h, HEADSZ)
            kc[h] = dot_nt(sel[...], kvt[pl.ds(r, HEADSZ), :]).astype(BF16)
            vc[h] = dot_nt(sel[...], kvt[pl.ds(aligned(C + r, HEADSZ), HEADSZ), :]).astype(BF16)
            scores = dot_nn(kc[h], qt[pl.ds(r, HEADSZ), :])
            for t in range(TOK // 128):
                flat[pl.ds(aligned((h * 8 + t) * KEYC, 8), KEYC), :] = scores[:, 128 * t : 128 * (t + 1)]

            def tile(t, carry):
                ls = pl.ds(aligned(128 * t, 128), 128)
                at = pl.ds(aligned((h * 8 + t) * KEYC, 8), KEYC)
                s = flat[at, :]
                rows = lax.broadcasted_iota(jnp.int32, (KEYC, 128), 0)
                s = jnp.where(rows < KEYS, s, -jnp.inf)
                top = jnp.max(s, 0, keepdims=True)
                p = jnp.exp2((s - top) * (LOG2E * HEADSZ**-0.5))
                p = p * (1.0 / jnp.sum(p, 0, keepdims=True))
                flat[at, :] = p
                attb[h, :, ls] = p.astype(BF16)
                return carry

            lax.fori_loop(0, TOK // 128, tile, 0)
            vt_h = kvc[pl.ds(aligned(C + r, HEADSZ), HEADSZ), :]
            mt[pl.ds(r, HEADSZ), :] = dot_nn(vt_h, attb[h]).astype(BF16)
            return carry

        lax.fori_loop(0, HEADS, head_forward, 0)
        yt[...] = xt[...] + (dot_nn(wot[...], mt[...]) + vt[:, V_OB : V_OB + 1])
        mean, inv = ln_stats(yt, TOK)
        stat[2], stat[3] = mean, inv
        ln_apply(yt, hgt.at[1], mean, inv, vt, V_MG, V_MB)
        gt = hgt.at[1]
        acc[...] = yt[...] + vt[:, V_DB : V_DB + 1]
        dgt[...] = jnp.zeros(dgt.shape, F32)
        lane16 = (lanes & 15) < HALF
        keep = (lane16, lane16 & (lanes < 96))

        def block(c, carry):
            span = pl.ds(aligned(BLK * c, BLK), BLK)
            e_s[...] = dot_nn(wut[span, :], gt[...])
            du_s[...] = dot_nn(wd[span, :], dzt[...])

            def group(i, carry):
                row = aligned(16 * i, 16)
                u_parts, de_parts = [], []
                for half in range(2):
                    r = aligned(row + 8 * half, 8)
                    chan = aligned(BLK * c + r, 8)
                    table = ht[pl.ds(chan, 8), :]
                    w = [jnp.broadcast_to(table[:, k : k + 1], (8, 128)) for k in range(11)]
                    taps = [w[1:4], w[4:7], w[7:10]]
                    flipped = [[w[9], w[8], w[7]], [w[6], w[5], w[4]], [w[3], w[2], w[1]]]
                    e = {}
                    for k in range(4):
                        e[k // 2, k % 2] = [
                            jnp.where(
                                keep[q],
                                e_s[pl.ds(r, 8), SLAB * k + 128 * q : SLAB * k + 128 * (q + 1)] + w[0],
                                0.0,
                            )
                            for q in range(2)
                        ]
                    views = side_views(e)
                    d = conv(views, taps, w[10], low, high)
                    dd, us = {}, []
                    for k in range(4):
                        out = []
                        for q in range(2):
                            value, slope = gelu_parts(d[k // 2, k % 2][q])
                            us.append(value)
                            out.append(
                                du_s[pl.ds(r, 8), SLAB * k + 128 * q : SLAB * k + 128 * (q + 1)] * slope
                            )
                        dd[k // 2, k % 2] = out
                    u_parts.append(us)
                    gsum = None
                    for k in range(4):
                        for q in range(2):
                            v = dd[k // 2, k % 2][q]
                            gsum = v if gsum is None else gsum + v
                    gh[10, pl.ds(chan, 8), :] += gsum
                    sums = tap_grads(views, dd, low, high)
                    for k in range(9):
                        gh[k + 1, pl.ds(chan, 8), :] += sums[k // 3][k % 3]
                    de = conv(side_views(dd), flipped, None, low, high)
                    des = [
                        jnp.where(keep[q], de[k // 2, k % 2][q], 0.0) for k in range(4) for q in range(2)
                    ]
                    de_parts.append(des)
                esums = [None, None]
                for k in range(8):
                    ls = slice(128 * k, 128 * (k + 1))
                    u_s[pl.ds(row, 16), ls] = jnp.concatenate(
                        [u_parts[0][k], u_parts[1][k]], 0
                    ).astype(BF16)
                    de16 = jnp.concatenate([de_parts[0][k], de_parts[1][k]], 0).astype(BF16)
                    de_s[pl.ds(row, 16), ls] = de16
                    wide = de16.astype(F32)
                    for half in range(2):
                        v = wide[8 * half : 8 * half + 8]
                        esums[half] = v if esums[half] is None else esums[half] + v
                chan = aligned(BLK * c + row, 16)
                gh[0, pl.ds(chan, 8), :] += esums[0]
                gh[0, pl.ds(aligned(chan + 8, 8), 8), :] += esums[1]
                return carry

            lax.fori_loop(0, BLK // 16, group, 0)
            acc[...] += dot_nn(wdt[:, span], u_s[...])
            dgt[...] += dot_nn(wu[:, span], de_s[...])
            gwd[span, :] += dot_nt(u_s[...], dzt[...])
            gwu[:, span] += dot_nt(gt[...], de_s[...])
            return carry

        lax.fori_loop(0, NBLK, block, 0)
        dbt[...] = acc[...].astype(BF16)
        give(dbt, out_ref)

        def middle(row, parts):
            for half in range(2):
                r = aligned(row + 8 * half, 8)
                z = dzt[pl.ds(row, 16), :].astype(F32)[8 * half : 8 * half + 8]
                gv[V_DB, pl.ds(r, 8), :] += fold(z)
                parts[half] = parts[half] + z
            both = jnp.concatenate(parts, 0)
            acc[pl.ds(row, 16), :] = both
            low_part = both.astype(BF16)
            dbt[pl.ds(row, 16), :] = low_part
            wide = low_part.astype(F32)
            for half in range(2):
                r = aligned(row + 8 * half, 8)
                gv[V_OB, pl.ds(r, 8), :] += fold(wide[8 * half : 8 * half + 8])

        norm_back(dgt, yt, stat[2], stat[3], vt, V_MG, gv, V_MG, V_MB, middle)
        dmt[...] = dot_nn(wo[...], dbt[...]).astype(BF16)
        gwo[...] += dot_nt(mt[...], dbt[...])

        def head_backward(h, carry):
            r = aligned(HEADSZ * h, HEADSZ)
            hs = pl.ds(r, HEADSZ)
            da = e_s.at[pl.ds(0, KEYC), :]
            da[...] = dot_nn(vc[h], dmt[hs, :])

            def tile(t, carry):
                ls = pl.ds(aligned(128 * t, 128), 128)
                p = flat[pl.ds(aligned((h * 8 + t) * KEYC, 8), KEYC), :]
                g = da[:, ls]
                total = jnp.sum(p * g, 0, keepdims=True)
                dsb[:, ls] = (p * (g - total)).astype(BF16)
                return carry

            lax.fori_loop(0, TOK // 128, tile, 0)
            dkvc[pl.ds(aligned(C + r, HEADSZ), HEADSZ), :] = dot_nt(dmt[hs, :], attb[h]).astype(BF16)
            dqt[hs, :] = (dot_nn(kvc[hs, :], dsb[...]) * HEADSZ**-0.5).astype(BF16)
            dkvc[hs, :] = (dot_nt(qt[hs, :], dsb[...]) * HEADSZ**-0.5).astype(BF16)
            return carry

        lax.fori_loop(0, HEADS, head_backward, 0)
        kvt[...] = dot_nn(dkvc[...], sel[...]).astype(BF16)
        gwkv[...] += dot_nt(nt[...], kvt[...])
        dnt = dgt.at[:, pl.ds(0, SLAB)]
        dnt[...] = dot_nn(wkv[...], kvt[...])

        def vbias(i, carry):
            row = aligned(16 * i, 16)
            wide = kvt[pl.ds(aligned(C + row, 16), 16), :].astype(F32)
            gv[V_VB, pl.ds(row, 16), :] += fold(wide)
            return carry

        lax.fori_loop(0, C // 16, vbias, 0)

        def keys_out(row, parts):
            low_part = jnp.concatenate(parts, 0).astype(BF16)
            nt[pl.ds(row, 16), :] = low_part
            gv[V_RB, pl.ds(row, 16), :] += fold(low_part.astype(F32))

        norm_back(
            dnt, rt, stat[4, :, :SLAB], stat[5, :, :SLAB], vt, V_KG, gv, V_KG, V_KB, keys_out
        )
        for k in range(4):
            ls = slice(SLAB * k, SLAB * (k + 1))
            gwr[k] += dot_nt(ht_[:, ls], nt[...])
            dgt[:, ls] = dot_nn(wq[...], dqt[:, ls]) + dot_nn(wr[k], nt[...])
        gwq[...] += dot_nt(ht_[...], dqt[...])

        def qbias(i, carry):
            row = aligned(16 * i, 16)
            gv[V_QB, pl.ds(row, 16), :] += fold(dqt[pl.ds(row, 16), :].astype(F32))
            return carry

        lax.fori_loop(0, C // 16, qbias, 0)

        def final(row, parts):
            both = jnp.concatenate(parts, 0) + acc[pl.ds(row, 16), :]
            dbt[pl.ds(row, 16), :] = both.astype(BF16)

        norm_back(dgt, xt, stat[0], stat[1], vt, V_NG, gv, V_NG, V_NB, final)
        give(dbt, gin_ref)

    @pl.when(slot == pl.num_programs(0) - 1)
    def _():
        pack_grads(shard_rows, flat, xp, gwq, gwr, gwkv, gwo, gwu, gwd, gv, gh)
        copies = []
        for k in range(gflat.shape[0]):
            if k >= 2:
                copies[k - 2].wait()
            stage[k % 2] = flat[shard_rows * k : shard_rows * k + gflat.shape[1], :]
            copies.append(pltpu.make_async_copy(stage.at[k % 2], gflat.at[k], sem.at[k % 2]))
            copies[k].start()
        copies[-2].wait()
        copies[-1].wait()


def run_images(live, images, cotangent, gathered, shard_rows):
    slots = images.shape[0]
    count, padded = gathered.shape[:2]
    item = pl.BlockSpec((1, NTOK, C), lambda s, n: (jnp.minimum(s, n[0] - 1), 0, 0))
    out_item = pl.BlockSpec((1, NTOK, C), lambda s, n: (s, 0, 0))
    anywhere = pl.BlockSpec(memory_space=pl.ANY)
    wide = lambda *dims: pltpu.VMEM(dims, F32)
    thin = lambda *dims: pltpu.VMEM(dims, BF16)
    flat_rows = -(-(count * shard_rows + 24) // 8) * 8
    scratch = [
        thin(C, C), thin(4, C, C), thin(2 * C, C), thin(C, C), thin(HID, C), thin(C, HID),
        thin(C, C), thin(4, C, C), thin(C, 2 * C), thin(C, C), thin(C, HID), thin(HID, C),
        wide(C, 128), wide(HID, 128),
        wide(C, C), wide(4, C, C), wide(C, 2 * C), wide(C, C), wide(C, HID), wide(HID, C),
        wide(11, C, 128), wide(11, HID, 128),
        thin(C, C), thin(KEYC, SLAB), wide(flat_rows, 128), wide(3, NTOK, 128), wide(3, 1296, 128),
        wide(C, TOK), thin(C, TOK), thin(2, C, TOK), thin(C, TOK),
        thin(HEADS, KEYC, TOK), thin(C, TOK), wide(C, TOK),
        wide(C, TOK), wide(C, TOK), thin(C, TOK), thin(C, TOK), thin(C, TOK),
        wide(C, SLAB), thin(C, SLAB), thin(2 * C, SLAB), thin(2 * C, KEYC),
        thin(HEADS, KEYC, HEADSZ), thin(HEADS, KEYC, HEADSZ), thin(KEYC, TOK), thin(2 * C, KEYC),
        wide(BLK, TOK), wide(BLK, TOK), thin(BLK, TOK), thin(BLK, TOK), wide(6, 8, TOK),
        wide(2, padded, 128), pltpu.SemaphoreType.DMA((2,)),
    ]
    call = pl.pallas_call(
        functools.partial(image_kernel, shard_rows),
        out_shape=[jax.ShapeDtypeStruct(images.shape, BF16)] * 2
        + [jax.ShapeDtypeStruct((count, padded, 128), F32)],
        grid_spec=pltpu.PrefetchScalarGridSpec(
            num_scalar_prefetch=1,
            grid=(slots,),
            in_specs=[
                item, item,
                pl.BlockSpec(
                    gathered.shape, lambda s, n: (0, 0, 0), pipeline_mode=pl.Buffered(1)
                ),
            ],
            out_specs=[out_item, out_item, anywhere],
            scratch_shapes=scratch,
        ),
        compiler_params=pltpu.CompilerParams(
            dimension_semantics=("arbitrary",), vmem_limit_bytes=67043328
        ),
        name="image_block",
    )
    return call(live, images, cotangent, gathered)


MESH = pl.DeviceIdType.MESH


class Place:
    def __init__(self, dims):
        self.dp, self.fsdp = dims
        self.ny, self.nz = self.dp // 2, self.fsdp // 2
        dp, fsdp = lax.axis_index("dp"), lax.axis_index("fsdp")
        self.y, self.c = dp // 2, dp % 2
        self.z, self.x = fsdp // 2, fsdp % 2
        self.offsets = [(dy, dx) for dy in range(self.ny) for dx in range(2)]

    def at(self, dy=0, dc=0, dz=0, dx=0):
        y, c = (self.y + dy) % self.ny, (self.c + dc) % 2
        z, x = (self.z + dz) % self.nz, (self.x + dx) % 2
        return y * 2 + c, z * 2 + x

    def index(self, **move):
        dp, fsdp = self.at(**move)
        return dp * self.fsdp + fsdp

    def target(self, **move):
        dp, fsdp = self.at(**move)
        return {"dp": dp, "fsdp": fsdp}

    def peers(self):
        moves = [dict(dz=k) for k in range(1, self.nz)]
        moves += [dict(dy=dy, dx=dx) for dy, dx in self.offsets[1:]]
        return moves + [dict(dc=1)]

    def enter(self):
        barrier = pltpu.get_barrier_semaphore()
        moves = self.peers()
        for move in moves:
            pl.semaphore_signal(barrier, inc=1, device_id=self.target(**move), device_id_type=MESH)
        pl.semaphore_wait(barrier, len(moves))


def remote(src, dst, send, recv, target):
    return pltpu.make_async_remote_copy(
        src_ref=src, dst_ref=dst, send_sem=send, recv_sem=recv, device_id=target, device_id_type=MESH
    )


def gather_kernel(dims, low_ref, out_ref, send, recv):
    p = Place(dims)
    p.enter()
    started = []

    def push(src, slot, **move):
        cp = remote(src, out_ref.at[slot], send.at[len(started)], recv.at[slot], p.target(**move))
        cp.start()
        started.append(cp)

    def arrived(slot):
        remote(low_ref, out_ref.at[slot], send.at[0], recv.at[slot], p.target(dc=1)).wait_recv()

    mine = p.index()
    for dz in range(1, p.nz):
        push(low_ref, mine, dz=dz)
    out_ref[mine] = low_ref[...]
    for dz in range(p.nz):
        slot = p.index(dz=dz)
        if dz:
            arrived(slot)
        src = out_ref.at[slot] if dz else low_ref
        for dy, dx in p.offsets[1:]:
            push(src, slot, dy=dy, dx=dx)
        push(src, slot, dc=1)
    for dz in range(p.nz):
        for dy, dx in p.offsets[1:]:
            slot = p.index(dz=dz, dy=dy, dx=dx)
            arrived(slot)
            push(out_ref.at[slot], slot, dc=1)
    for dz in range(p.nz):
        for dy, dx in p.offsets:
            arrived(p.index(dz=dz, dy=dy, dx=dx, dc=1))
    for cp in started:
        cp.wait_send()


def all_weights(dims, low):
    count = dims[0] * dims[1]
    ny, nz = dims[0] // 2, dims[1] // 2
    sends = nz - 1 + nz * 2 * ny + nz * (2 * ny - 1)
    vmem = pl.BlockSpec(memory_space=pltpu.VMEM)
    return pl.pallas_call(
        functools.partial(gather_kernel, dims),
        out_shape=jax.ShapeDtypeStruct((count,) + low.shape, low.dtype),
        in_specs=[vmem],
        out_specs=vmem,
        scratch_shapes=[pltpu.SemaphoreType.DMA((sends,)), pltpu.SemaphoreType.DMA((count,))],
        compiler_params=pltpu.CompilerParams(
            collective_id=0, has_side_effects=True, vmem_limit_bytes=32 * 1024 * 1024
        ),
        name="weights_gather",
    )(low)


def scatter_kernel(dims, g_ref, out_ref, mine, other, sx, rx, sz, rz, lsem, csem, xsem, zsem):
    p = Place(dims)
    p.enter()
    n_xy = len(p.offsets)
    order = list(range(1, p.nz)) + [0]
    local, cross = {}, {}
    for dz in order:
        for k, (dy, dx) in enumerate(p.offsets):
            cp = remote(
                g_ref.at[p.index(dy=dy, dx=dx, dz=dz, dc=1)], other.at[dz, k],
                csem.at[0, dz, k], csem.at[1, dz, k], p.target(dc=1),
            )
            cp.start()
            cross[dz, k] = cp
            cp = pltpu.make_async_copy(
                g_ref.at[p.index(dy=dy, dx=dx, dz=dz)], mine.at[dz, k], lsem.at[dz, k]
            )
            cp.start()
            local[dz, k] = cp
    planar = {}
    waiting = None
    for dz in order:
        for k in list(range(1, n_xy)) + [0]:
            dy, dx = p.offsets[k]
            local[dz, k].wait()
            cross[dz, k].wait_recv()
            total = mine[dz, k] + other[dz, k]
            if k == 0:
                mine[dz, 0] = total
            else:
                sx[dz, k - 1] = total.astype(BF16)
            if waiting is not None:
                waiting.start()
                waiting = None
            if k:
                waiting = remote(
                    sx.at[dz, k - 1], rx.at[dz, k - 1],
                    xsem.at[0, dz, k - 1], xsem.at[1, dz, k - 1], p.target(dy=dy, dx=dx),
                )
                planar[dz, k] = waiting
    final = None
    lines = {}
    for dz in order:
        total = mine[dz, 0]
        for k in range(1, n_xy):
            planar[dz, k].wait_recv()
            total = total + rx[dz, k - 1].astype(F32)
        if dz:
            sz[dz - 1] = total.astype(BF16)
        else:
            final = total
        if waiting is not None:
            waiting.start()
            waiting = None
        if dz:
            waiting = remote(
                sz.at[dz - 1], rz.at[dz - 1], zsem.at[0, dz - 1], zsem.at[1, dz - 1], p.target(dz=dz)
            )
            lines[dz] = waiting
    for dz in range(1, p.nz):
        lines[dz].wait_recv()
        final = final + rz[dz - 1].astype(F32)
    out_ref[...] = final
    for group in (cross, planar, lines):
        for cp in group.values():
            cp.wait_send()


def sum_to_owner(dims, terms):
    ny, nz = dims[0] // 2, dims[1] // 2
    n_xy = 2 * ny
    rows = terms.shape[1]
    dma = pltpu.SemaphoreType.DMA
    return pl.pallas_call(
        functools.partial(scatter_kernel, dims),
        out_shape=jax.ShapeDtypeStruct((rows, 128), F32),
        in_specs=[pl.BlockSpec(memory_space=pl.ANY)],
        out_specs=pl.BlockSpec(memory_space=pltpu.VMEM),
        scratch_shapes=[
            pltpu.VMEM((nz, n_xy, rows, 128), F32),
            pltpu.VMEM((nz, n_xy, rows, 128), F32),
            pltpu.VMEM((nz, n_xy - 1, rows, 128), BF16),
            pltpu.VMEM((nz, n_xy - 1, rows, 128), BF16),
            pltpu.VMEM((nz - 1, rows, 128), BF16),
            pltpu.VMEM((nz - 1, rows, 128), BF16),
            dma((nz, n_xy)), dma((2, nz, n_xy)), dma((2, nz, n_xy - 1)), dma((2, nz - 1)),
        ],
        compiler_params=pltpu.CompilerParams(
            collective_id=1, has_side_effects=True, vmem_limit_bytes=48 * 1024 * 1024
        ),
        name="grads_scatter",
    )(terms)


def body(images, counts, cotangent, master, first_moment, second_moment, average):
    dims = (lax.axis_size("dp"), lax.axis_size("fsdp"))
    shard_rows = master.shape[0] // 128
    padded = -(-shard_rows // 16) * 16
    low = master.reshape(shard_rows, 128).astype(BF16)
    low = jnp.pad(low, ((0, padded - shard_rows), (0, 0)))
    gathered = all_weights(dims, low)
    output_images, grad_images, terms = run_images(
        counts, images, cotangent, gathered, shard_rows
    )
    grads = sum_to_owner(dims, terms)[:shard_rows].reshape(-1)
    new_first = beta_first * first_moment + (1.0 - beta_first) * grads
    new_second = beta_second * second_moment + (1.0 - beta_second) * grads * grads
    fix_first = 1.0 - beta_first**STEP
    fix_second = 1.0 - beta_second**STEP
    step_size = (
        new_first / fix_first / (jnp.sqrt(new_second / fix_second) + adam_eps)
        + weight_decay * master
    )
    new_master = master - learn_rate * step_size
    new_average = ema_keep * average + (1.0 - ema_keep) * new_master
    return (
        grads,
        new_first,
        new_second,
        new_master,
        new_average,
        new_master.astype(jnp.bfloat16),
        output_images,
        grad_images,
    )


def solution(mesh):
    return jax.shard_map(
        body,
        mesh=mesh,
        in_specs=(
            P(("dp", "fsdp"), None, None),
            P(("dp", "fsdp")),
            P(("dp", "fsdp"), None, None),
            P(("dp", "fsdp")),
            P(("dp", "fsdp")),
            P(("dp", "fsdp")),
            P(("dp", "fsdp")),
        ),
        out_specs=(
            P(("dp", "fsdp")),
            P(("dp", "fsdp")),
            P(("dp", "fsdp")),
            P(("dp", "fsdp")),
            P(("dp", "fsdp")),
            P(("dp", "fsdp")),
            P(("dp", "fsdp"), None, None),
            P(("dp", "fsdp"), None, None),
        ),
        check_vma=False,
    )
```

```python
import functools
import math

import jax
import jax.numpy as jnp
import numpy as np
from jax import lax
from jax.experimental import pallas as pl
from jax.experimental.pallas import tpu as pltpu
from jax.sharding import PartitionSpec as P

C = 320
HEADS = 5
HEADSZ = 64
HID = 1280
SIDE = 28
STEP = 3
HALF = 14
NTOK = 784
KEYS = 196


norm_eps = 1e-06
adam_eps = 1e-08
learn_rate = 0.02
weight_decay = 0.05
beta_first = 0.5
beta_second = 0.5
ema_keep = 0.9


CAP = 6
TOK = 1024
SLAB = 256
KEYC = 208
BLK = 256
NBLK = HID // BLK
F32 = jnp.float32
BF16 = jnp.bfloat16
ERFC_C = 0.35
ERFC_P = (
    0.1397766380054567,
    0.13686603367482672,
    0.1431944963239702,
    0.00881332607675965,
    0.2112475588897874,
    -0.18454519984085327,
    0.04464718332154041,
)
LOG2E = 1.4426950408889634
V_NG, V_NB, V_QB, V_RB, V_KG, V_KB, V_VB, V_OB, V_MG, V_MB, V_DB = range(11)


def dot_nn(left, right):
    return lax.dot_general(left, right, (((1,), (0,)), ((), ())), preferred_element_type=F32)


def dot_nt(left, right):
    return lax.dot_general(left, right, (((1,), (1,)), ((), ())), preferred_element_type=F32)


def fold(x):
    total = x[:, :128]
    for k in range(1, x.shape[1] // 128):
        total = total + x[:, 128 * k : 128 * (k + 1)]
    return total


def aligned(value, step):
    return pl.multiple_of(value, step)


def column(ref, row, lane):
    return ref[pl.ds(row, 8), :][:, lane : lane + 1]


def ln_stats(src, width):
    def first(i, acc):
        return acc + src[pl.ds(aligned(8 * i, 8), 8), :]

    acc = lax.fori_loop(0, C // 8, first, jnp.zeros((8, width), F32), unroll=4)
    mean = jnp.broadcast_to(jnp.sum(acc, 0, keepdims=True) * (1.0 / C), (8, width))

    def second(i, acc):
        d = src[pl.ds(aligned(8 * i, 8), 8), :] - mean
        return acc + d * d

    acc = lax.fori_loop(0, C // 8, second, jnp.zeros((8, width), F32), unroll=4)
    inv = lax.rsqrt(jnp.sum(acc, 0, keepdims=True) * (1.0 / C) + norm_eps)
    return mean, jnp.broadcast_to(inv, (8, width))


def ln_apply(src, dst, mean, inv, vt, gain_lane, bias_lane):
    def step(i, carry):
        row = aligned(16 * i, 16)
        parts = []
        for half in range(2):
            r = aligned(row + 8 * half, 8)
            u = (src[pl.ds(r, 8), :] - mean) * inv
            parts.append(u * column(vt, r, gain_lane) + column(vt, r, bias_lane))
        dst[pl.ds(row, 16), :] = jnp.concatenate(parts, 0).astype(BF16)
        return carry

    lax.fori_loop(0, C // 16, step, 0, unroll=2)


def norm_back(grad, src, mean, inv, vt, gain_lane, gv, gain_slot, bias_slot, emit):
    width = mean.shape[1]

    def first(i, carry):
        acc_one, acc_two = carry
        r = aligned(8 * i, 8)
        u = (src[pl.ds(r, 8), :] - mean) * inv
        d = grad[pl.ds(r, 8), :]
        du = d * u
        gain = column(vt, r, gain_lane)
        gv[gain_slot, pl.ds(r, 8), :] += fold(du)
        gv[bias_slot, pl.ds(r, 8), :] += fold(d)
        return acc_one + d * gain, acc_two + du * gain

    zero = jnp.zeros((8, width), F32)
    acc_one, acc_two = lax.fori_loop(0, C // 8, first, (zero, zero), unroll=2)
    m_one = jnp.broadcast_to(jnp.sum(acc_one, 0, keepdims=True) * (1.0 / C), (8, width))
    m_two = jnp.broadcast_to(jnp.sum(acc_two, 0, keepdims=True) * (1.0 / C), (8, width))

    def second(i, carry):
        row = aligned(16 * i, 16)
        parts = []
        for half in range(2):
            r = aligned(row + 8 * half, 8)
            u = (src[pl.ds(r, 8), :] - mean) * inv
            d = grad[pl.ds(r, 8), :] * column(vt, r, gain_lane)
            parts.append(inv * (d - m_one - u * m_two))
        emit(row, parts)
        return carry

    lax.fori_loop(0, C // 16, second, 0)


def shift_down(v, low):
    a, b = pltpu.roll(v[0], 16, 1), pltpu.roll(v[1], 16, 1)
    return [jnp.where(low, b, a), jnp.where(low, a, b)]


def shift_up(v, high):
    a, b = pltpu.roll(v[0], 112, 1), pltpu.roll(v[1], 112, 1)
    return [jnp.where(high, b, a), jnp.where(high, a, b)]


def side_views(e):
    views = {}
    for a in range(2):
        left = [pltpu.roll(v, 1, 1) for v in e[a, 1]]
        right = [pltpu.roll(v, 127, 1) for v in e[a, 0]]
        views[a, 0] = (left, e[a, 0], e[a, 1])
        views[a, 1] = (e[a, 0], e[a, 1], right)
    return views


def conv(views, taps, bias, low, high):
    def combo(a, b, row):
        out = []
        for h in range(2):
            t = views[a, b][0][h] * taps[row][0]
            t = t + views[a, b][1][h] * taps[row][1]
            out.append(t + views[a, b][2][h] * taps[row][2])
        return out

    result = {}
    for b in range(2):
        top = shift_down(combo(1, b, 0), low)
        mid, bot = combo(0, b, 1), combo(1, b, 2)
        result[0, b] = [top[h] + mid[h] + bot[h] for h in range(2)]
        top, mid = combo(0, b, 0), combo(1, b, 1)
        bot = shift_up(combo(0, b, 2), high)
        result[1, b] = [top[h] + mid[h] + bot[h] for h in range(2)]
        if bias is not None:
            for a in range(2):
                result[a, b] = [v + bias for v in result[a, b]]
    return result


def tap_grads(views, dd, low, high):
    sums = [[None] * 3 for _ in range(3)]
    for b in range(2):
        up = shift_up(dd[0, b], high)
        down = shift_down(dd[1, b], low)
        pairs = ((up, views[1, b], dd[1, b], views[0, b]),
                 (dd[0, b], views[0, b], dd[1, b], views[1, b]),
                 (dd[0, b], views[1, b], down, views[0, b]))
        for row in range(3):
            g_one, v_one, g_two, v_two = pairs[row]
            for col in range(3):
                t = sums[row][col]
                for h in range(2):
                    p = g_one[h] * v_one[col][h] + g_two[h] * v_two[col][h]
                    t = p if t is None else t + p
                sums[row][col] = t
    return sums


def gelu_parts(z):
    t = 1.0 / (1.0 + ERFC_C * jnp.abs(z))
    poly = ERFC_P[6]
    for k in range(5, -1, -1):
        poly = poly * t + ERFC_P[k]
    e = jnp.exp2(z * z * (-0.5 * LOG2E))
    q = poly * t * e
    phi = jnp.where(z < 0, q, 1.0 - q)
    return z * phi, phi + z * e * (1.0 / math.sqrt(2.0 * math.pi))


ROW_QUERY, ROW_REDUCE, ROW_KEYS, ROW_KV = 0, 805, 4010, 4015
ROW_VALUE, ROW_UP, ROW_HID, ROW_DOWN = 5615, 6425, 9625, 9735


def rows_from_flat(flat, base, pairs, buf):
    left = lax.broadcasted_iota(jnp.int32, (8, 128), 1) < 64

    def step(i, carry):
        t = [flat[pl.ds(base + 40 * i + k, 8, stride=5), :] for k in range(5)]
        r = [pltpu.roll(t[k], 64, 1) for k in range(2, 5)]
        even = (t[0], t[1], t[2])
        odd = (jnp.where(left, r[0], r[1]), jnp.where(left, r[1], r[2]), r[2])
        for k in range(3):
            buf.at[k][pl.ds(16 * i, 8, stride=2), :] = even[k]
            buf.at[k][pl.ds(16 * i + 1, 8, stride=2), :] = odd[k]
        return carry

    lax.fori_loop(0, -(-pairs // 8), step, 0)


def rows_to_flat(flat, base, pairs, buf):
    left = lax.broadcasted_iota(jnp.int32, (8, 128), 1) < 64

    def emit(i, size):
        even = [buf.at[k][pl.ds(16 * i, size, stride=2), :] for k in range(3)]
        odd = [buf.at[k][pl.ds(16 * i + 1, size, stride=2), :] for k in range(3)]
        r = [pltpu.roll(odd[k], 64, 1) for k in range(3)]
        lo = left[:size]
        t = (even[0], even[1], jnp.where(lo, even[2], r[0]),
             jnp.where(lo, r[0], r[1]), jnp.where(lo, r[1], r[2]))
        for k in range(5):
            flat[pl.ds(base + 40 * i + k, size, stride=5), :] = t[k]

    def step(i, carry):
        emit(i, 8)
        return carry

    lax.fori_loop(0, pairs // 8, step, 0)
    if pairs % 8:
        emit(pairs // 8, pairs % 8)


def buf_rows(buf, start, size):
    at = slice(start, start + size)
    return jnp.concatenate([buf[0, at], buf[1, at], buf[2, at][:, :64]], 1)


def put_rows(buf, start, value):
    at = slice(start, start + value.shape[0])
    buf[0, at] = value[:, :128]
    buf[1, at] = value[:, 128:256]
    buf[2, at, :64] = value[:, 256:]


def unpack_weights(
    shard_rows, wall, parts, psem, flat, buf, eye,
    wqt, wrt, wkvt, wot, wut, wdt, wq, wr, wkv, wo, wu, wd, vt, ht,
):
    groups = wall.shape[0] // 8
    loads = [
        pltpu.make_async_copy(wall.at[pl.ds(8 * g, 8)], parts.at[g % 2], psem.at[g % 2])
        for g in range(groups)
    ]
    loads[0].start()
    for g in range(groups):
        if g + 1 < groups:
            loads[g + 1].start()
        loads[g].wait()
        for k in range(8):
            at = shard_rows * (8 * g + k)
            flat[at : at + shard_rows, :] = parts[g % 2, k, :shard_rows].astype(F32)
    tail = shard_rows * wall.shape[0]
    flat[tail:, :] = jnp.zeros((flat.shape[0] - tail, 128), F32)
    vectors = {}

    def vector(slot, row):
        vectors[slot] = [buf[t, row : row + 1, :] for t in range(3)]

    def flip(w):
        return dot_nt(eye[: w.shape[1], : w.shape[1]], w).astype(BF16)

    rows_from_flat(flat, ROW_QUERY, 161, buf)
    wq[...] = buf_rows(buf, 2, C).astype(BF16)
    vector(V_NG, 0)
    vector(V_NB, 1)
    wqt[...] = flip(wq[...])
    rows_from_flat(flat, ROW_REDUCE, 641, buf)
    for k in range(4):
        wr[k] = buf_rows(buf, 1 + C * k, C).astype(BF16)
        wrt[k] = flip(wr[k])
    vector(V_QB, 0)
    vector(V_RB, 1281)
    rows_from_flat(flat, ROW_KEYS, 1, buf)
    vector(V_KG, 0)
    vector(V_KB, 1)
    for k in range(5):
        cols = flat[pl.ds(ROW_KV + k, C, stride=5), :]
        wkv[:, 128 * k : 128 * (k + 1)] = cols.astype(BF16)
        wkvt[128 * k : 128 * (k + 1), :] = flip(wkv[:, 128 * k : 128 * (k + 1)])
    rows_from_flat(flat, ROW_VALUE, 162, buf)
    wo[...] = buf_rows(buf, 1, C).astype(BF16)
    wot[...] = flip(wo[...])
    vector(V_VB, 0)
    vector(V_OB, 321)
    vector(V_MG, 322)
    vector(V_MB, 323)
    for k in range(10):
        cols = flat[pl.ds(ROW_UP + k, C, stride=10), :]
        wu[:, 128 * k : 128 * (k + 1)] = cols.astype(BF16)
        wut[128 * k : 128 * (k + 1), :] = flip(wu[:, 128 * k : 128 * (k + 1)])
    rows_from_flat(flat, ROW_DOWN, 641, buf)
    for k in range(5):
        at = slice(BLK * k, BLK * (k + 1))
        wd[at, :] = buf_rows(buf, BLK * k, BLK).astype(BF16)
        wdt[:, at] = flip(wd[at, :])
    vector(V_DB, 1280)
    for t in range(3):
        rows = jnp.concatenate([vectors[k][t] for k in range(11)] + [jnp.zeros((117, 128), F32)], 0)
        size = min(128, C - 128 * t)
        vt[128 * t : 128 * t + size, :] = rows.T[:size]
    for k in range(10):
        rows = flat[pl.ds(ROW_HID + k, 11, stride=10), :]
        rows = jnp.concatenate([rows, jnp.zeros((117, 128), F32)], 0)
        ht[128 * k : 128 * (k + 1), :] = rows.T


def pack_grads(shard_rows, flat, buf, gwq, gwr, gwkv, gwo, gwu, gwd, gv, gh):
    flat[ROW_DOWN + 3200 :, :] = jnp.zeros((flat.shape[0] - ROW_DOWN - 3200, 128), F32)

    def vector(slot, row):
        for t in range(3):
            size = min(128, C - 128 * t)
            part = gv[slot, 128 * t : 128 * t + size, :]
            if size < 128:
                part = jnp.concatenate([part, jnp.zeros((128 - size, 128), F32)], 0)
            buf[t, row : row + 1, :] = jnp.sum(part.T, 0, keepdims=True)

    put_rows(buf, 2, gwq[...])
    vector(V_NG, 0)
    vector(V_NB, 1)
    rows_to_flat(flat, ROW_QUERY, 161, buf)
    for k in range(4):
        put_rows(buf, 1 + C * k, gwr[k])
    vector(V_QB, 0)
    vector(V_RB, 1281)
    rows_to_flat(flat, ROW_REDUCE, 641, buf)
    vector(V_KG, 0)
    vector(V_KB, 1)
    rows_to_flat(flat, ROW_KEYS, 1, buf)
    for k in range(5):
        flat[pl.ds(ROW_KV + k, C, stride=5), :] = gwkv[:, 128 * k : 128 * (k + 1)]
    put_rows(buf, 1, gwo[...])
    vector(V_VB, 0)
    vector(V_OB, 321)
    vector(V_MG, 322)
    vector(V_MB, 323)
    rows_to_flat(flat, ROW_VALUE, 162, buf)
    for k in range(10):
        flat[pl.ds(ROW_UP + k, C, stride=10), :] = gwu[:, 128 * k : 128 * (k + 1)]
        for slot in range(11):
            part = gh[slot, 128 * k : 128 * (k + 1), :]
            at = ROW_HID + 10 * slot + k
            flat[at : at + 1, :] = jnp.sum(part.T, 0, keepdims=True)
    put_rows(buf, 0, gwd[...])
    vector(V_DB, 1280)
    for t in range(3):
        buf[t, 1281:1282, :] = jnp.zeros((1, 128), F32)
    rows_to_flat(flat, ROW_DOWN, 641, buf)
    half = ROW_DOWN + 3202
    flat[half : half + 1, 64:] = jnp.zeros((1, 64), F32)
    flat[half + 1 :, :] = jnp.zeros((flat.shape[0] - half - 1, 128), F32)


def image_kernel(
    shard_rows, work, x_ref, ct_ref, pool_ref, wall,
    out_ref, gin_ref, done_ref, gflat,
    wqt, wrt, wkvt, wot, wut, wdt, wq, wr, wkv, wo, wu, wd, vt, ht,
    gwq, gwr, gwkv, gwo, gwu, gwd, gv, gh,
    eye, sel, perm, flat, xp, xt, dzt, hgt, qt, attb, mt, yt, acc, dgt, dbt, dmt, dqt,
    rt, nt, kvt, kvc, kc, vc, dsb, dkvc, e_s, du_s, u_s, de_s, stat, stage, sem, parts, psem,
):
    slot = pl.program_id(0)
    own, live = work[1], work[2]
    lanes = lax.broadcasted_iota(jnp.int32, (8, 128), 1)
    low, high = lanes < 16, lanes >= 112

    @pl.when(slot == 0)
    def _():
        for ref in (gwq, gwr, gwkv, gwo, gwu, gwd, gv, gh):
            ref[...] = jnp.zeros(ref.shape, ref.dtype)
        r = lax.broadcasted_iota(jnp.int32, (C, C), 0)
        c = lax.broadcasted_iota(jnp.int32, (C, C), 1)
        eye[...] = (r == c).astype(F32).astype(BF16)
        r = lax.broadcasted_iota(jnp.int32, (KEYC, SLAB), 0)
        c = lax.broadcasted_iota(jnp.int32, (KEYC, SLAB), 1)
        i, j = c >> 4, c & 15
        hit = (r == i * HALF + j) & (i < HALF) & (j < HALF)
        sel[...] = hit.astype(F32).astype(BF16)
        unpack_weights(
            shard_rows, wall, parts, psem, flat, xp, eye,
            wqt, wrt, wkvt, wot, wut, wdt, wq, wr, wkv, wo, wu, wd, vt, ht,
        )
        for k in range(8):
            r = lax.broadcasted_iota(jnp.int32, (128, NTOK), 0) + 128 * k
            c = lax.broadcasted_iota(jnp.int32, (128, NTOK), 1)
            i, j = (r >> 4) & 15, r & 15
            want = (2 * i + (r >> 9)) * SIDE + 2 * j + ((r >> 8) & 1)
            hit = (c == want) & (i < HALF) & (j < HALF)
            perm[128 * k : 128 * (k + 1), :] = hit.astype(F32).astype(BF16)

    def take(src, dst):
        for k in range(4):
            ks = slice(SLAB * k, SLAB * (k + 1))
            dst[:, ks] = dot_nt(src[...], perm[ks, :]).astype(dst.dtype)

    def give(src, own_dst, part):
        acc[:, :NTOK] = dot_nn(src[...], perm[...])

        @pl.when(slot < own)
        def _():
            own_dst[0] = acc[:, :NTOK].astype(BF16)

        @pl.when(slot >= own)
        def _():
            done_ref[0, part] = acc[:, :NTOK].astype(BF16)

    @pl.when(slot < live)
    def _():
        @pl.when(slot < own)
        def _():
            take(x_ref.at[0], xt)
            take(ct_ref.at[0], dzt)

        @pl.when(slot >= own)
        def _():
            take(pool_ref.at[0, 0], xt)
            take(pool_ref.at[0, 1], dzt)

        mean, inv = ln_stats(xt, TOK)
        stat[0], stat[1] = mean, inv
        ln_apply(xt, hgt.at[0], mean, inv, vt, V_NG, V_NB)
        ht_ = hgt.at[0]
        qt[...] = (dot_nn(wqt[...], ht_[...]) + vt[:, V_QB : V_QB + 1]).astype(BF16)
        reduced = vt[:, V_RB : V_RB + 1]
        for k in range(4):
            reduced = reduced + dot_nn(wrt[k], ht_[:, SLAB * k : SLAB * (k + 1)])
        rt[...] = reduced
        kmean, kinv = ln_stats(rt, SLAB)
        stat[4, :, :SLAB], stat[5, :, :SLAB] = kmean, kinv
        ln_apply(rt, nt, kmean, kinv, vt, V_KG, V_KB)
        kvt[:C, :] = dot_nn(wkvt[:C, :], nt[...]).astype(BF16)
        kvt[C:, :] = (dot_nn(wkvt[C:, :], nt[...]) + vt[:, V_VB : V_VB + 1]).astype(BF16)
        kvc[...] = dot_nt(kvt[...], sel[...]).astype(BF16)

        def head_forward(h, carry):
            r = aligned(HEADSZ * h, HEADSZ)
            kc[h] = dot_nt(sel[...], kvt[pl.ds(r, HEADSZ), :]).astype(BF16)
            vc[h] = dot_nt(sel[...], kvt[pl.ds(aligned(C + r, HEADSZ), HEADSZ), :]).astype(BF16)
            scores = dot_nn(kc[h], qt[pl.ds(r, HEADSZ), :])
            for t in range(TOK // 128):
                flat[pl.ds(aligned((h * 8 + t) * KEYC, 8), KEYC), :] = scores[:, 128 * t : 128 * (t + 1)]

            def tile(t, carry):
                ls = pl.ds(aligned(128 * t, 128), 128)
                at = pl.ds(aligned((h * 8 + t) * KEYC, 8), KEYC)
                s = flat[at, :]
                rows = lax.broadcasted_iota(jnp.int32, (KEYC, 128), 0)
                s = jnp.where(rows < KEYS, s, -jnp.inf)
                top = jnp.max(s, 0, keepdims=True)
                p = jnp.exp2((s - top) * (LOG2E * HEADSZ**-0.5))
                p = p * (1.0 / jnp.sum(p, 0, keepdims=True))
                flat[at, :] = p
                attb[h, :, ls] = p.astype(BF16)
                return carry

            lax.fori_loop(0, TOK // 128, tile, 0)
            vt_h = kvc[pl.ds(aligned(C + r, HEADSZ), HEADSZ), :]
            mt[pl.ds(r, HEADSZ), :] = dot_nn(vt_h, attb[h]).astype(BF16)
            return carry

        lax.fori_loop(0, HEADS, head_forward, 0)
        yt[...] = xt[...] + (dot_nn(wot[...], mt[...]) + vt[:, V_OB : V_OB + 1])
        mean, inv = ln_stats(yt, TOK)
        stat[2], stat[3] = mean, inv
        ln_apply(yt, hgt.at[1], mean, inv, vt, V_MG, V_MB)
        gt = hgt.at[1]
        acc[...] = yt[...] + vt[:, V_DB : V_DB + 1]
        dgt[...] = jnp.zeros(dgt.shape, F32)
        lane16 = (lanes & 15) < HALF
        keep = (lane16, lane16 & (lanes < 96))

        def block(c, carry):
            span = pl.ds(aligned(BLK * c, BLK), BLK)
            e_s[...] = dot_nn(wut[span, :], gt[...])
            du_s[...] = dot_nn(wd[span, :], dzt[...])

            def group(i, carry):
                row = aligned(16 * i, 16)
                u_parts, de_parts = [], []
                for half in range(2):
                    r = aligned(row + 8 * half, 8)
                    chan = aligned(BLK * c + r, 8)
                    table = ht[pl.ds(chan, 8), :]
                    w = [jnp.broadcast_to(table[:, k : k + 1], (8, 128)) for k in range(11)]
                    taps = [w[1:4], w[4:7], w[7:10]]
                    flipped = [[w[9], w[8], w[7]], [w[6], w[5], w[4]], [w[3], w[2], w[1]]]
                    e = {}
                    for k in range(4):
                        e[k // 2, k % 2] = [
                            jnp.where(
                                keep[q],
                                e_s[pl.ds(r, 8), SLAB * k + 128 * q : SLAB * k + 128 * (q + 1)] + w[0],
                                0.0,
                            )
                            for q in range(2)
                        ]
                    views = side_views(e)
                    d = conv(views, taps, w[10], low, high)
                    dd, us = {}, []
                    for k in range(4):
                        out = []
                        for q in range(2):
                            value, slope = gelu_parts(d[k // 2, k % 2][q])
                            us.append(value)
                            out.append(
                                du_s[pl.ds(r, 8), SLAB * k + 128 * q : SLAB * k + 128 * (q + 1)] * slope
                            )
                        dd[k // 2, k % 2] = out
                    u_parts.append(us)
                    gsum = None
                    for k in range(4):
                        for q in range(2):
                            v = dd[k // 2, k % 2][q]
                            gsum = v if gsum is None else gsum + v
                    gh[10, pl.ds(chan, 8), :] += gsum
                    sums = tap_grads(views, dd, low, high)
                    for k in range(9):
                        gh[k + 1, pl.ds(chan, 8), :] += sums[k // 3][k % 3]
                    de = conv(side_views(dd), flipped, None, low, high)
                    des = [
                        jnp.where(keep[q], de[k // 2, k % 2][q], 0.0) for k in range(4) for q in range(2)
                    ]
                    de_parts.append(des)
                esums = [None, None]
                for k in range(8):
                    ls = slice(128 * k, 128 * (k + 1))
                    u_s[pl.ds(row, 16), ls] = jnp.concatenate(
                        [u_parts[0][k], u_parts[1][k]], 0
                    ).astype(BF16)
                    de16 = jnp.concatenate([de_parts[0][k], de_parts[1][k]], 0).astype(BF16)
                    de_s[pl.ds(row, 16), ls] = de16
                    wide = de16.astype(F32)
                    for half in range(2):
                        v = wide[8 * half : 8 * half + 8]
                        esums[half] = v if esums[half] is None else esums[half] + v
                chan = aligned(BLK * c + row, 16)
                gh[0, pl.ds(chan, 8), :] += esums[0]
                gh[0, pl.ds(aligned(chan + 8, 8), 8), :] += esums[1]
                return carry

            lax.fori_loop(0, BLK // 16, group, 0)
            acc[...] += dot_nn(wdt[:, span], u_s[...])
            dgt[...] += dot_nn(wu[:, span], de_s[...])
            gwd[span, :] += dot_nt(u_s[...], dzt[...])
            gwu[:, span] += dot_nt(gt[...], de_s[...])
            return carry

        lax.fori_loop(0, NBLK, block, 0)
        dbt[...] = acc[...].astype(BF16)
        give(dbt, out_ref, 0)

        def middle(row, parts):
            for half in range(2):
                r = aligned(row + 8 * half, 8)
                z = dzt[pl.ds(row, 16), :].astype(F32)[8 * half : 8 * half + 8]
                gv[V_DB, pl.ds(r, 8), :] += fold(z)
                parts[half] = parts[half] + z
            both = jnp.concatenate(parts, 0)
            acc[pl.ds(row, 16), :] = both
            low_part = both.astype(BF16)
            dbt[pl.ds(row, 16), :] = low_part
            wide = low_part.astype(F32)
            for half in range(2):
                r = aligned(row + 8 * half, 8)
                gv[V_OB, pl.ds(r, 8), :] += fold(wide[8 * half : 8 * half + 8])

        norm_back(dgt, yt, stat[2], stat[3], vt, V_MG, gv, V_MG, V_MB, middle)
        dmt[...] = dot_nn(wo[...], dbt[...]).astype(BF16)
        gwo[...] += dot_nt(mt[...], dbt[...])

        def head_backward(h, carry):
            r = aligned(HEADSZ * h, HEADSZ)
            hs = pl.ds(r, HEADSZ)
            da = e_s.at[pl.ds(0, KEYC), :]
            da[...] = dot_nn(vc[h], dmt[hs, :])

            def tile(t, carry):
                ls = pl.ds(aligned(128 * t, 128), 128)
                p = flat[pl.ds(aligned((h * 8 + t) * KEYC, 8), KEYC), :]
                g = da[:, ls]
                total = jnp.sum(p * g, 0, keepdims=True)
                dsb[:, ls] = (p * (g - total)).astype(BF16)
                return carry

            lax.fori_loop(0, TOK // 128, tile, 0)
            dkvc[pl.ds(aligned(C + r, HEADSZ), HEADSZ), :] = dot_nt(dmt[hs, :], attb[h]).astype(BF16)
            dqt[hs, :] = (dot_nn(kvc[hs, :], dsb[...]) * HEADSZ**-0.5).astype(BF16)
            dkvc[hs, :] = (dot_nt(qt[hs, :], dsb[...]) * HEADSZ**-0.5).astype(BF16)
            return carry

        lax.fori_loop(0, HEADS, head_backward, 0)
        kvt[...] = dot_nn(dkvc[...], sel[...]).astype(BF16)
        gwkv[...] += dot_nt(nt[...], kvt[...])
        dnt = dgt.at[:, pl.ds(0, SLAB)]
        dnt[...] = dot_nn(wkv[...], kvt[...])

        def vbias(i, carry):
            row = aligned(16 * i, 16)
            wide = kvt[pl.ds(aligned(C + row, 16), 16), :].astype(F32)
            gv[V_VB, pl.ds(row, 16), :] += fold(wide)
            return carry

        lax.fori_loop(0, C // 16, vbias, 0)

        def keys_out(row, parts):
            low_part = jnp.concatenate(parts, 0).astype(BF16)
            nt[pl.ds(row, 16), :] = low_part
            gv[V_RB, pl.ds(row, 16), :] += fold(low_part.astype(F32))

        norm_back(
            dnt, rt, stat[4, :, :SLAB], stat[5, :, :SLAB], vt, V_KG, gv, V_KG, V_KB, keys_out
        )
        for k in range(4):
            ls = slice(SLAB * k, SLAB * (k + 1))
            gwr[k] += dot_nt(ht_[:, ls], nt[...])
            dgt[:, ls] = dot_nn(wq[...], dqt[:, ls]) + dot_nn(wr[k], nt[...])
        gwq[...] += dot_nt(ht_[...], dqt[...])

        def qbias(i, carry):
            row = aligned(16 * i, 16)
            gv[V_QB, pl.ds(row, 16), :] += fold(dqt[pl.ds(row, 16), :].astype(F32))
            return carry

        lax.fori_loop(0, C // 16, qbias, 0)

        def final(row, parts):
            both = jnp.concatenate(parts, 0) + acc[pl.ds(row, 16), :]
            dbt[pl.ds(row, 16), :] = both.astype(BF16)

        norm_back(dgt, xt, stat[0], stat[1], vt, V_NG, gv, V_NG, V_NB, final)
        give(dbt, gin_ref, 1)

    @pl.when(slot == pl.num_programs(0) - 1)
    def _():
        pack_grads(shard_rows, flat, xp, gwq, gwr, gwkv, gwo, gwu, gwd, gv, gh)
        copies = []
        for k in range(gflat.shape[0]):
            if k >= 2:
                copies[k - 2].wait()
            stage[k % 2] = flat[shard_rows * k : shard_rows * k + gflat.shape[1], :]
            copies.append(pltpu.make_async_copy(stage.at[k % 2], gflat.at[k], sem.at[k % 2]))
            copies[k].start()
        copies[-2].wait()
        copies[-1].wait()


def run_images(work, images, cotangent, pool, gathered, shard_rows):
    count, padded = gathered.shape[:2]
    item = pl.BlockSpec(
        (1, C, NTOK), lambda s, w: (jnp.maximum(jnp.minimum(s, w[1] - 1), 0), 0, 0)
    )
    foreign = pl.BlockSpec(
        (1, 2, C, NTOK),
        lambda s, w: (w[3 + jnp.clip(jnp.minimum(s, w[2] - 1) - w[1], 0, POOL - 1)], 0, 0, 0),
    )
    once = pl.BlockSpec(foreign.block_shape, foreign.index_map, pipeline_mode=pl.Buffered(1))
    anywhere = pl.BlockSpec(memory_space=pl.ANY)
    wide = lambda *dims: pltpu.VMEM(dims, F32)
    thin = lambda *dims: pltpu.VMEM(dims, BF16)
    flat_rows = -(-(count * shard_rows + 24) // 8) * 8
    scratch = [
        thin(C, C), thin(4, C, C), thin(2 * C, C), thin(C, C), thin(HID, C), thin(C, HID),
        thin(C, C), thin(4, C, C), thin(C, 2 * C), thin(C, C), thin(C, HID), thin(HID, C),
        wide(C, 128), wide(HID, 128),
        wide(C, C), wide(4, C, C), wide(C, 2 * C), wide(C, C), wide(C, HID), wide(HID, C),
        wide(11, C, 128), wide(11, HID, 128),
        thin(C, C), thin(KEYC, SLAB), thin(TOK, NTOK), wide(flat_rows, 128), wide(3, 1296, 128),
        wide(C, TOK), thin(C, TOK), thin(2, C, TOK), thin(C, TOK),
        thin(HEADS, KEYC, TOK), thin(C, TOK), wide(C, TOK),
        wide(C, TOK), wide(C, TOK), thin(C, TOK), thin(C, TOK), thin(C, TOK),
        wide(C, SLAB), thin(C, SLAB), thin(2 * C, SLAB), thin(2 * C, KEYC),
        thin(HEADS, KEYC, HEADSZ), thin(HEADS, KEYC, HEADSZ), thin(KEYC, TOK), thin(2 * C, KEYC),
        wide(BLK, TOK), wide(BLK, TOK), thin(BLK, TOK), thin(BLK, TOK), wide(6, 8, TOK),
        wide(2, padded, 128), pltpu.SemaphoreType.DMA((2,)),
        thin(2, 8, padded, 128), pltpu.SemaphoreType.DMA((2,)),
    ]
    call = pl.pallas_call(
        functools.partial(image_kernel, shard_rows),
        out_shape=[jax.ShapeDtypeStruct(images.shape, BF16)] * 2
        + [jax.ShapeDtypeStruct(pool.shape, BF16), jax.ShapeDtypeStruct((count, padded, 128), F32)],
        grid_spec=pltpu.PrefetchScalarGridSpec(
            num_scalar_prefetch=1,
            grid=(CAP + pool.shape[0],),
            in_specs=[
                item, item, once,
                anywhere,
            ],
            out_specs=[item, item, foreign, anywhere],
            scratch_shapes=scratch,
        ),
        compiler_params=pltpu.CompilerParams(
            dimension_semantics=("arbitrary",), vmem_limit_bytes=67043328
        ),
        name="image_block",
    )
    return call(work, images, cotangent, pool, gathered)


MESH = pl.DeviceIdType.MESH


class Place:
    def __init__(self, dims):
        self.dp, self.fsdp = dims
        self.ny, self.nz = self.dp // 2, self.fsdp // 2
        dp, fsdp = lax.axis_index("dp"), lax.axis_index("fsdp")
        self.y, self.c = dp // 2, dp % 2
        self.z, self.x = fsdp // 2, fsdp % 2
        self.offsets = [(dy, dx) for dy in range(self.ny) for dx in range(2)]

    def at(self, dy=0, dc=0, dz=0, dx=0):
        y, c = (self.y + dy) % self.ny, (self.c + dc) % 2
        z, x = (self.z + dz) % self.nz, (self.x + dx) % 2
        return y * 2 + c, z * 2 + x

    def index(self, **move):
        dp, fsdp = self.at(**move)
        return dp * self.fsdp + fsdp

    def target(self, **move):
        dp, fsdp = self.at(**move)
        return {"dp": dp, "fsdp": fsdp}

    def peers(self):
        moves = [dict(dz=k) for k in range(1, self.nz)]
        moves += [dict(dy=dy, dx=dx) for dy, dx in self.offsets[1:]]
        return moves + [dict(dc=1)]

    def enter(self):
        barrier = pltpu.get_barrier_semaphore()
        moves = self.peers()
        for move in moves:
            pl.semaphore_signal(barrier, inc=1, device_id=self.target(**move), device_id_type=MESH)
        pl.semaphore_wait(barrier, len(moves))


def remote(src, dst, send, recv, target):
    return pltpu.make_async_remote_copy(
        src_ref=src, dst_ref=dst, send_sem=send, recv_sem=recv, device_id=target, device_id_type=MESH
    )


def gather_kernel(dims, low_ref, out_ref, send, recv):
    p = Place(dims)
    p.enter()
    started = []

    def push(src, slot, **move):
        cp = remote(src, out_ref.at[slot], send.at[len(started)], recv.at[slot], p.target(**move))
        cp.start()
        started.append(cp)

    def arrived(slot):
        remote(low_ref, out_ref.at[slot], send.at[0], recv.at[slot], p.target(dc=1)).wait_recv()

    mine = p.index()
    for dz in range(1, p.nz):
        push(low_ref, mine, dz=dz)
    out_ref[mine] = low_ref[...]
    for dz in range(p.nz):
        slot = p.index(dz=dz)
        if dz:
            arrived(slot)
        src = out_ref.at[slot] if dz else low_ref
        for dy, dx in p.offsets[1:]:
            push(src, slot, dy=dy, dx=dx)
        push(src, slot, dc=1)
    for dz in range(p.nz):
        for dy, dx in p.offsets[1:]:
            slot = p.index(dz=dz, dy=dy, dx=dx)
            arrived(slot)
            push(out_ref.at[slot], slot, dc=1)
    for dz in range(p.nz):
        for dy, dx in p.offsets:
            arrived(p.index(dz=dz, dy=dy, dx=dx, dc=1))
    for cp in started:
        cp.wait_send()


def all_weights(dims, low):
    count = dims[0] * dims[1]
    ny, nz = dims[0] // 2, dims[1] // 2
    sends = nz - 1 + nz * 2 * ny + nz * (2 * ny - 1)
    vmem = pl.BlockSpec(memory_space=pltpu.VMEM)
    return pl.pallas_call(
        functools.partial(gather_kernel, dims),
        out_shape=jax.ShapeDtypeStruct((count,) + low.shape, low.dtype),
        in_specs=[vmem],
        out_specs=vmem,
        scratch_shapes=[pltpu.SemaphoreType.DMA((sends,)), pltpu.SemaphoreType.DMA((count,))],
        compiler_params=pltpu.CompilerParams(
            collective_id=0, has_side_effects=True, vmem_limit_bytes=32 * 1024 * 1024
        ),
        name="weights_gather",
    )(low)


def scatter_kernel(dims, g_ref, out_ref, mine, other, sx, rx, sz, rz, lsem, csem, xsem, zsem):
    p = Place(dims)
    p.enter()
    n_xy = len(p.offsets)
    order = list(range(1, p.nz)) + [0]
    local, cross = {}, {}
    for dz in order:
        for k, (dy, dx) in enumerate(p.offsets):
            cp = remote(
                g_ref.at[p.index(dy=dy, dx=dx, dz=dz, dc=1)], other.at[dz, k],
                csem.at[0, dz, k], csem.at[1, dz, k], p.target(dc=1),
            )
            cp.start()
            cross[dz, k] = cp
            cp = pltpu.make_async_copy(
                g_ref.at[p.index(dy=dy, dx=dx, dz=dz)], mine.at[dz, k], lsem.at[dz, k]
            )
            cp.start()
            local[dz, k] = cp
    planar = {}
    waiting = None
    for dz in order:
        for k in list(range(1, n_xy)) + [0]:
            dy, dx = p.offsets[k]
            local[dz, k].wait()
            cross[dz, k].wait_recv()
            total = mine[dz, k] + other[dz, k]
            if k == 0:
                mine[dz, 0] = total
            else:
                sx[dz, k - 1] = total.astype(BF16)
            if waiting is not None:
                waiting.start()
                waiting = None
            if k:
                waiting = remote(
                    sx.at[dz, k - 1], rx.at[dz, k - 1],
                    xsem.at[0, dz, k - 1], xsem.at[1, dz, k - 1], p.target(dy=dy, dx=dx),
                )
                planar[dz, k] = waiting
    final = None
    lines = {}
    for dz in order:
        total = mine[dz, 0]
        for k in range(1, n_xy):
            planar[dz, k].wait_recv()
            total = total + rx[dz, k - 1].astype(F32)
        if dz:
            sz[dz - 1] = total.astype(BF16)
        else:
            final = total
        if waiting is not None:
            waiting.start()
            waiting = None
        if dz:
            waiting = remote(
                sz.at[dz - 1], rz.at[dz - 1], zsem.at[0, dz - 1], zsem.at[1, dz - 1], p.target(dz=dz)
            )
            lines[dz] = waiting
    for dz in range(1, p.nz):
        lines[dz].wait_recv()
        final = final + rz[dz - 1].astype(F32)
    out_ref[...] = final
    for group in (cross, planar, lines):
        for cp in group.values():
            cp.wait_send()


def sum_to_owner(dims, terms):
    ny, nz = dims[0] // 2, dims[1] // 2
    n_xy = 2 * ny
    rows = terms.shape[1]
    dma = pltpu.SemaphoreType.DMA
    return pl.pallas_call(
        functools.partial(scatter_kernel, dims),
        out_shape=jax.ShapeDtypeStruct((rows, 128), F32),
        in_specs=[pl.BlockSpec(memory_space=pl.ANY)],
        out_specs=pl.BlockSpec(memory_space=pltpu.VMEM),
        scratch_shapes=[
            pltpu.VMEM((nz, n_xy, rows, 128), F32),
            pltpu.VMEM((nz, n_xy, rows, 128), F32),
            pltpu.VMEM((nz, n_xy - 1, rows, 128), BF16),
            pltpu.VMEM((nz, n_xy - 1, rows, 128), BF16),
            pltpu.VMEM((nz - 1, rows, 128), BF16),
            pltpu.VMEM((nz - 1, rows, 128), BF16),
            dma((nz, n_xy)), dma((2, nz, n_xy)), dma((2, nz, n_xy - 1)), dma((2, nz - 1)),
        ],
        compiler_params=pltpu.CompilerParams(
            collective_id=1, has_side_effects=True, vmem_limit_bytes=48 * 1024 * 1024
        ),
        name="grads_scatter",
    )(terms)


MOVES = 4
RELAYS = 3
POOL = MOVES + RELAYS


@functools.lru_cache(maxsize=None)
def routing(ny, nz, variants=8):
    chips = ny * nz * 2
    at = lambda y, z, x: (y * nz + z) * 2 + x
    edges = []
    for y in range(ny):
        for z in range(nz):
            edges.append((at(y, z, 0), at(y, z, 1), 0, 0))
            for x in range(2):
                if y % 2 == 0 and y + 1 < ny:
                    edges.append((at(y, z, x), at(y + 1, z, x), 1, 1))
                if z < nz - 1:
                    edges.append((at(y, z, x), at(y, z + 1, x), 2, 3))
    count = len(edges)
    incidence = np.zeros((count, chips))
    sides = np.zeros((MOVES, chips, count), np.float32)
    for e, (u, v, du, dv) in enumerate(edges):
        incidence[e, u], incidence[e, v] = 1, -1
        sides[du, u, e], sides[dv, v, e] = 1, -1
    ideal = incidence @ np.linalg.pinv(incidence.T @ incidence)
    rng = np.random.default_rng(7)
    guess, exact, fix = [], [], []
    for variant in range(variants):
        order = rng.permutation(count)
        root = list(range(chips))

        def find(a):
            while root[a] != a:
                a = root[a]
            return a

        tree = []
        for e in order:
            a, b = find(edges[e][0]), find(edges[e][1])
            if a != b:
                root[a] = b
                tree.append(e)
        others = [e for e in range(count) if e not in tree]
        near = {k: [] for k in range(chips)}
        for e in tree:
            near[edges[e][0]].append((edges[e][1], e))
            near[edges[e][1]].append((edges[e][0], e))
        a_mat, b_mat = np.zeros((count, chips)), np.zeros((count, count))
        for e in tree:
            side, todo = {edges[e][0]}, [edges[e][0]]
            while todo:
                for b, via in near[todo.pop()]:
                    if via != e and b not in side:
                        side.add(b)
                        todo.append(b)
            a_mat[e, list(side)] = 1
            for q in others:
                b_mat[e, q] = (edges[q][1] in side) * 1 - (edges[q][0] in side) * 1
        g_mat = np.zeros((count, chips))
        for q in others:
            b_mat[q, q] = 1
            g_mat[q] = ideal[q]
        guess.append(g_mat)
        exact.append(a_mat)
        fix.append(b_mat)
    stack = lambda items: np.stack(items).astype(np.float32)
    return stack(guess), stack(exact), stack(fix), sides


def plan(dims, counts):
    ny, nz = dims[0] // 2, dims[1] // 2
    guess, exact, fix, sides = routing(ny, nz)
    chips = ny * nz * 2
    c = counts.reshape(ny, 2, nz, 2).transpose(0, 2, 3, 1).reshape(chips, 2)
    total = jnp.sum(c, 1).astype(F32)
    excess = total - jnp.sum(total) / chips
    high = lax.Precision.HIGHEST
    near = jnp.round(jnp.einsum("tek,k->te", guess, excess, precision=high))
    flow = jnp.einsum("tek,k->te", exact, excess, precision=high)
    flow = jnp.round(flow + jnp.einsum("teq,tq->te", fix, near, precision=high))
    cost = jnp.sum(jnp.maximum(jnp.abs(flow) - 2.0, 0.0) + 0.001 * jnp.abs(flow), 1)
    best = flow[jnp.argmin(cost)]
    out = jnp.clip(jnp.einsum("dke,e->dk", sides, best, precision=high), 0, 2).astype(jnp.int32)
    left = [c[:, 0], c[:, 1]]
    takes, order = {}, {}
    for d in (2, 3, 0, 1):
        bigger = left[0] >= left[1]
        both, one = out[d] == 2, out[d] == 1
        t = [
            (both | (one & bigger)) & (left[0] > 0),
            (both | (one & ~bigger)) & (left[1] > 0),
        ]
        t = [v.astype(jnp.int32) for v in t]
        left = [left[0] - t[0], left[1] - t[1]]
        takes[d] = jnp.stack(t, 1)
        order[d] = jnp.stack(left, 1)
    kept = jnp.stack(left, 1)
    grid = lambda v: v.reshape(ny, nz, 2, 2)
    zero = jnp.zeros((ny, 1, 2, 2), jnp.int32)
    got = [
        grid(takes[0])[:, :, ::-1],
        grid(takes[1]).reshape(ny // 2, 2, nz, 2, 2)[:, ::-1].reshape(ny, nz, 2, 2),
        jnp.concatenate([zero, grid(takes[2])[:, :-1]], 1),
        jnp.concatenate([grid(takes[3])[:, 1:], zero], 1),
    ]
    got = [v.reshape(chips, 2) for v in got]
    load = kept + got[0] + got[1] + got[2] + got[3]
    give = jnp.clip((load - load[:, ::-1]) // 2, 0, RELAYS)
    take_in = give[:, ::-1]
    dp, fsdp = lax.axis_index("dp"), lax.axis_index("fsdp")
    me = ((dp // 2) * nz + fsdp // 2) * 2 + fsdp % 2
    pack = jnp.stack(
        [c, kept, load, give, take_in]
        + [takes[d] for d in range(MOVES)]
        + [order[d] for d in range(MOVES)]
        + got,
        0,
    )
    mine = lax.dynamic_slice(pack, (0, me, dp % 2), (pack.shape[0], 1, 1)).reshape(-1)
    have, keep, items, send, accept = (mine[k] for k in range(5))
    taken, place, came = mine[5:9], mine[9:13], mine[13:17]
    stay = items - send
    send_index = jnp.clip(place, 0, CAP - 1)
    rank = keep + jnp.cumsum(came) - came
    entry = stay + jnp.arange(RELAYS)
    from_move = jnp.sum(
        jnp.where((rank[None] == entry[:, None]) & (came[None] > 0), jnp.arange(MOVES)[None], 0), 1
    )
    relay_index = jnp.where(entry < keep, jnp.clip(entry, 0, CAP - 1), CAP + from_move)
    own = jnp.minimum(keep, stay)
    item = own + jnp.arange(POOL)
    from_item = jnp.sum(
        jnp.where((rank[None] == item[:, None]) & (came[None] > 0), jnp.arange(MOVES)[None], 0), 1
    )
    foreign = jnp.where(item < stay, from_item, jnp.clip(MOVES + item - stay, 0, POOL - 1))
    bring = jnp.concatenate([send_index, relay_index]).astype(jnp.int32)
    work = jnp.concatenate(
        [jnp.stack([jnp.maximum(stay + accept, 1), own, stay + accept]), foreign]
    ).astype(jnp.int32)
    back = jnp.where(rank < stay, jnp.arange(MOVES), POOL + jnp.clip(rank - stay, 0, RELAYS - 1))
    slot = jnp.arange(CAP)
    sent = jnp.sum(
        jnp.where((place[None] == slot[:, None]) & (taken[None] > 0), jnp.arange(MOVES)[None], 0), 1
    )
    source = jnp.where(
        slot >= keep,
        CAP + sent,
        jnp.where(slot >= stay, CAP + MOVES + jnp.clip(slot - stay, 0, RELAYS - 1), slot),
    )
    home = jnp.concatenate([back, source, (slot < have).astype(jnp.int32)]).astype(jnp.int32)
    return bring, work, home


def move_targets(p):
    return ((p.target(dx=1), None), (p.target(dy=1 - 2 * (p.y % 2)), None),
            (p.target(dz=1), p.z < p.nz - 1), (p.target(dz=-1), p.z > 0))


def guarded(cond, action):
    if cond is None:
        action()
    else:
        pl.when(cond)(action)


def greet(p):
    barrier = pltpu.get_barrier_semaphore()

    def signal(target):
        pl.semaphore_signal(barrier, inc=1, device_id=target, device_id_type=MESH)

    for target, cond in move_targets(p):
        guarded(cond, lambda target=target: signal(target))
    signal(p.target(dc=1))
    inner = (p.z < p.nz - 1).astype(jnp.int32) + (p.z > 0).astype(jnp.int32)
    pl.semaphore_wait(barrier, 3 + inner)


def bring_kernel(dims, tbl, x_ref, ct_ref, pool, stage, landed, relay, msem, rsem):
    p = Place(dims)
    greet(p)
    targets = move_targets(p)
    arriving = (None, None, p.z > 0, p.z < p.nz - 1)
    for d in range(MOVES):
        stage[d, 0] = x_ref[tbl[d]]
        stage[d, 1] = ct_ref[tbl[d]]
    copies = [
        remote(stage.at[d], landed.at[d], msem.at[0, d], msem.at[1, d], targets[d][0])
        for d in range(MOVES)
    ]
    for d in range(MOVES):
        guarded(targets[d][1], copies[d].start)
    for d in range(MOVES):
        guarded(arriving[d], copies[d].wait_recv)
    for j in range(RELAYS):
        pick = tbl[MOVES + j]
        own, got = jnp.minimum(pick, CAP - 1), jnp.maximum(pick - CAP, 0)
        for part, ref in enumerate((x_ref, ct_ref)):
            relay[j, part] = jnp.where(pick < CAP, ref[own], landed[got, part])
    passed = [
        remote(relay.at[j], pool.at[MOVES + j], rsem.at[0, j], rsem.at[1, j], p.target(dc=1))
        for j in range(RELAYS)
    ]
    for cp in passed:
        cp.start()
    for d in range(MOVES):
        pool[d] = landed[d]
    for cp in passed:
        cp.wait_recv()
    for cp in passed:
        cp.wait_send()
    for d in range(MOVES):
        guarded(targets[d][1], copies[d].wait_send)


def bring_images(dims, table, images, cotangent):
    vmem = pl.BlockSpec(memory_space=pltpu.VMEM)
    item = (2,) + images.shape[1:]
    dma = pltpu.SemaphoreType.DMA
    return pl.pallas_call(
        functools.partial(bring_kernel, dims),
        out_shape=jax.ShapeDtypeStruct((POOL,) + item, BF16),
        in_specs=[pl.BlockSpec(memory_space=pltpu.SMEM), vmem, vmem],
        out_specs=vmem,
        scratch_shapes=[
            pltpu.VMEM((MOVES,) + item, BF16), pltpu.VMEM((MOVES,) + item, BF16),
            pltpu.VMEM((RELAYS,) + item, BF16), dma((2, MOVES)), dma((2, RELAYS)),
        ],
        compiler_params=pltpu.CompilerParams(
            collective_id=2, has_side_effects=True, vmem_limit_bytes=56 * 1024 * 1024
        ),
        name="bring_images",
    )(table, images, cotangent)


def home_kernel(dims, tbl, own_out, own_grad, done, out_ref, gin_ref, core, stage, back, csem, bsem):
    p = Place(dims)
    greet(p)
    targets = move_targets(p)
    routes = ((targets[0][0], None), (targets[1][0], None), targets[3], targets[2])
    arriving = (None, None, targets[2][1], targets[3][1])
    passed = [
        remote(done.at[MOVES + j], core.at[j], csem.at[0, j], csem.at[1, j], p.target(dc=1))
        for j in range(RELAYS)
    ]
    for cp in passed:
        cp.start()
    for cp in passed:
        cp.wait_recv()
    for d in range(MOVES):
        pick = tbl[d]
        here, there = jnp.minimum(pick, POOL - 1), jnp.maximum(pick - POOL, 0)
        for part in range(2):
            stage[d, part] = jnp.where(pick < POOL, done[here, part], core[there, part])
    copies = [
        remote(stage.at[d], back.at[d], bsem.at[0, d], bsem.at[1, d], routes[d][0])
        for d in range(MOVES)
    ]
    for d in range(MOVES):
        guarded(routes[d][1], copies[d].start)
    for d in range(MOVES):
        guarded(arriving[d], copies[d].wait_recv)
    for s in range(CAP):
        pick, live = tbl[MOVES + s], tbl[MOVES + CAP + s]
        mine = jnp.minimum(pick, CAP - 1)
        moved = jnp.clip(pick - CAP, 0, MOVES - 1)
        passed_on = jnp.maximum(pick - CAP - MOVES, 0)
        for part, (own, dst) in enumerate(((own_out, out_ref), (own_grad, gin_ref))):
            value = jnp.where(
                pick < CAP,
                own[mine],
                jnp.where(pick < CAP + MOVES, back[moved, part], core[passed_on, part]),
            )
            dst[s] = jnp.where(live > 0, value, jnp.zeros_like(value))
    for cp in passed:
        cp.wait_send()
    for d in range(MOVES):
        guarded(routes[d][1], copies[d].wait_send)


def bring_home(dims, table, own_out, own_grad, done):
    vmem = pl.BlockSpec(memory_space=pltpu.VMEM)
    item = (2,) + own_out.shape[1:]
    dma = pltpu.SemaphoreType.DMA
    return pl.pallas_call(
        functools.partial(home_kernel, dims),
        out_shape=[jax.ShapeDtypeStruct(own_out.shape, BF16)] * 2,
        in_specs=[pl.BlockSpec(memory_space=pltpu.SMEM), vmem, vmem, vmem],
        out_specs=[vmem, vmem],
        scratch_shapes=[
            pltpu.VMEM((RELAYS,) + item, BF16), pltpu.VMEM((MOVES,) + item, BF16),
            pltpu.VMEM((MOVES,) + item, BF16), dma((2, RELAYS)), dma((2, MOVES)),
        ],
        compiler_params=pltpu.CompilerParams(
            collective_id=3, has_side_effects=True, vmem_limit_bytes=60 * 1024 * 1024
        ),
        name="bring_home",
    )(table, own_out, own_grad, done)


def body(images, counts, cotangent, master, first_moment, second_moment, average):
    dims = (lax.axis_size("dp"), lax.axis_size("fsdp"))
    shard_rows = master.shape[0] // 128
    padded = -(-(shard_rows + 1) // 16) * 16
    low = jnp.concatenate(
        [
            master.reshape(shard_rows, 128).astype(BF16),
            jnp.broadcast_to(counts.astype(BF16)[:, None], (1, 128)),
            jnp.zeros((padded - shard_rows - 1, 128), BF16),
        ],
        0,
    )
    gathered = all_weights(dims, low)
    bring, work, home = plan(dims, gathered[:, shard_rows, 0].astype(jnp.int32))
    flip = lambda v: jnp.swapaxes(v, 1, 2)
    images, cotangent = flip(images), flip(cotangent)
    pool = bring_images(dims, bring, images, cotangent)
    own_out, own_grad, done, terms = run_images(
        work, images, cotangent, pool, gathered, shard_rows
    )
    output_images, grad_images = bring_home(dims, home, own_out, own_grad, done)
    output_images, grad_images = flip(output_images), flip(grad_images)
    grads = sum_to_owner(dims, terms)[:shard_rows].reshape(-1)
    new_first = beta_first * first_moment + (1.0 - beta_first) * grads
    new_second = beta_second * second_moment + (1.0 - beta_second) * grads * grads
    fix_first = 1.0 - beta_first**STEP
    fix_second = 1.0 - beta_second**STEP
    step_size = (
        new_first / fix_first / (jnp.sqrt(new_second / fix_second) + adam_eps)
        + weight_decay * master
    )
    new_master = master - learn_rate * step_size
    new_average = ema_keep * average + (1.0 - ema_keep) * new_master
    return (
        grads,
        new_first,
        new_second,
        new_master,
        new_average,
        new_master.astype(jnp.bfloat16),
        output_images,
        grad_images,
    )


def solution(mesh):
    return jax.shard_map(
        body,
        mesh=mesh,
        in_specs=(
            P(("dp", "fsdp"), None, None),
            P(("dp", "fsdp")),
            P(("dp", "fsdp"), None, None),
            P(("dp", "fsdp")),
            P(("dp", "fsdp")),
            P(("dp", "fsdp")),
            P(("dp", "fsdp")),
        ),
        out_specs=(
            P(("dp", "fsdp")),
            P(("dp", "fsdp")),
            P(("dp", "fsdp")),
            P(("dp", "fsdp")),
            P(("dp", "fsdp")),
            P(("dp", "fsdp")),
            P(("dp", "fsdp"), None, None),
            P(("dp", "fsdp"), None, None),
        ),
        check_vma=False,
    )
```

```python
import functools
import math

import jax
import jax.numpy as jnp
import numpy as np
from jax import lax
from jax.experimental import pallas as pl
from jax.experimental.pallas import tpu as pltpu
from jax.sharding import PartitionSpec as P

C = 320
HEADS = 5
HEADSZ = 64
HID = 1280
SIDE = 28
STEP = 3
HALF = 14
NTOK = 784
KEYS = 196


norm_eps = 1e-06
adam_eps = 1e-08
learn_rate = 0.02
weight_decay = 0.05
beta_first = 0.5
beta_second = 0.5
ema_keep = 0.9


CAP = 6
TOK = 1024
SLAB = 256
KEYC = 208
BLK = 256
NBLK = HID // BLK
F32 = jnp.float32
BF16 = jnp.bfloat16
ERFC_C = 0.35
ERFC_P = (
    0.1397766380054567,
    0.13686603367482672,
    0.1431944963239702,
    0.00881332607675965,
    0.2112475588897874,
    -0.18454519984085327,
    0.04464718332154041,
)
LOG2E = 1.4426950408889634
V_NG, V_NB, V_QB, V_RB, V_KG, V_KB, V_VB, V_OB, V_MG, V_MB, V_DB = range(11)


def dot_nn(left, right):
    return lax.dot_general(left, right, (((1,), (0,)), ((), ())), preferred_element_type=F32)


def dot_nt(left, right):
    return lax.dot_general(left, right, (((1,), (1,)), ((), ())), preferred_element_type=F32)


def fold(x):
    total = x[:, :128]
    for k in range(1, x.shape[1] // 128):
        total = total + x[:, 128 * k : 128 * (k + 1)]
    return total


def aligned(value, step):
    return pl.multiple_of(value, step)


def column(ref, row, lane):
    return ref[pl.ds(row, 8), :][:, lane : lane + 1]


def ln_stats(src, width):
    def first(i, acc):
        return acc + src[pl.ds(aligned(8 * i, 8), 8), :]

    acc = lax.fori_loop(0, C // 8, first, jnp.zeros((8, width), F32), unroll=4)
    mean = jnp.broadcast_to(jnp.sum(acc, 0, keepdims=True) * (1.0 / C), (8, width))

    def second(i, acc):
        d = src[pl.ds(aligned(8 * i, 8), 8), :] - mean
        return acc + d * d

    acc = lax.fori_loop(0, C // 8, second, jnp.zeros((8, width), F32), unroll=4)
    inv = lax.rsqrt(jnp.sum(acc, 0, keepdims=True) * (1.0 / C) + norm_eps)
    return mean, jnp.broadcast_to(inv, (8, width))


def ln_apply(src, dst, mean, inv, vt, gain_lane, bias_lane):
    def step(i, carry):
        row = aligned(16 * i, 16)
        parts = []
        for half in range(2):
            r = aligned(row + 8 * half, 8)
            u = (src[pl.ds(r, 8), :] - mean) * inv
            parts.append(u * column(vt, r, gain_lane) + column(vt, r, bias_lane))
        dst[pl.ds(row, 16), :] = jnp.concatenate(parts, 0).astype(BF16)
        return carry

    lax.fori_loop(0, C // 16, step, 0, unroll=2)


def norm_back(grad, src, mean, inv, vt, gain_lane, gv, gain_slot, bias_slot, emit):
    width = mean.shape[1]

    def first(i, carry):
        acc_one, acc_two = carry
        r = aligned(8 * i, 8)
        u = (src[pl.ds(r, 8), :] - mean) * inv
        d = grad[pl.ds(r, 8), :]
        du = d * u
        gain = column(vt, r, gain_lane)
        gv[gain_slot, pl.ds(r, 8), :] += fold(du)
        gv[bias_slot, pl.ds(r, 8), :] += fold(d)
        return acc_one + d * gain, acc_two + du * gain

    zero = jnp.zeros((8, width), F32)
    acc_one, acc_two = lax.fori_loop(0, C // 8, first, (zero, zero), unroll=2)
    m_one = jnp.broadcast_to(jnp.sum(acc_one, 0, keepdims=True) * (1.0 / C), (8, width))
    m_two = jnp.broadcast_to(jnp.sum(acc_two, 0, keepdims=True) * (1.0 / C), (8, width))

    def second(i, carry):
        row = aligned(16 * i, 16)
        parts = []
        for half in range(2):
            r = aligned(row + 8 * half, 8)
            u = (src[pl.ds(r, 8), :] - mean) * inv
            d = grad[pl.ds(r, 8), :] * column(vt, r, gain_lane)
            parts.append(inv * (d - m_one - u * m_two))
        emit(row, parts)
        return carry

    lax.fori_loop(0, C // 16, second, 0)


def shift_down(v, low):
    a, b = pltpu.roll(v[0], 16, 1), pltpu.roll(v[1], 16, 1)
    return [jnp.where(low, b, a), jnp.where(low, a, b)]


def shift_up(v, high):
    a, b = pltpu.roll(v[0], 112, 1), pltpu.roll(v[1], 112, 1)
    return [jnp.where(high, b, a), jnp.where(high, a, b)]


def side_views(e):
    views = {}
    for a in range(2):
        left = [pltpu.roll(v, 1, 1) for v in e[a, 1]]
        right = [pltpu.roll(v, 127, 1) for v in e[a, 0]]
        views[a, 0] = (left, e[a, 0], e[a, 1])
        views[a, 1] = (e[a, 0], e[a, 1], right)
    return views


def conv(views, taps, bias, low, high):
    def combo(a, b, row):
        out = []
        for h in range(2):
            t = views[a, b][0][h] * taps[row][0]
            t = t + views[a, b][1][h] * taps[row][1]
            out.append(t + views[a, b][2][h] * taps[row][2])
        return out

    result = {}
    for b in range(2):
        top = shift_down(combo(1, b, 0), low)
        mid, bot = combo(0, b, 1), combo(1, b, 2)
        result[0, b] = [top[h] + mid[h] + bot[h] for h in range(2)]
        top, mid = combo(0, b, 0), combo(1, b, 1)
        bot = shift_up(combo(0, b, 2), high)
        result[1, b] = [top[h] + mid[h] + bot[h] for h in range(2)]
        if bias is not None:
            for a in range(2):
                result[a, b] = [v + bias for v in result[a, b]]
    return result


def tap_grads(views, dd, low, high):
    sums = [[None] * 3 for _ in range(3)]
    for b in range(2):
        up = shift_up(dd[0, b], high)
        down = shift_down(dd[1, b], low)
        pairs = ((up, views[1, b], dd[1, b], views[0, b]),
                 (dd[0, b], views[0, b], dd[1, b], views[1, b]),
                 (dd[0, b], views[1, b], down, views[0, b]))
        for row in range(3):
            g_one, v_one, g_two, v_two = pairs[row]
            for col in range(3):
                t = sums[row][col]
                for h in range(2):
                    p = g_one[h] * v_one[col][h] + g_two[h] * v_two[col][h]
                    t = p if t is None else t + p
                sums[row][col] = t
    return sums


def gelu_parts(z):
    t = 1.0 / (1.0 + ERFC_C * jnp.abs(z))
    poly = ERFC_P[6]
    for k in range(5, -1, -1):
        poly = poly * t + ERFC_P[k]
    e = jnp.exp2(z * z * (-0.5 * LOG2E))
    q = poly * t * e
    phi = jnp.where(z < 0, q, 1.0 - q)
    return z * phi, phi + z * e * (1.0 / math.sqrt(2.0 * math.pi))


ROW_QUERY, ROW_REDUCE, ROW_KEYS, ROW_KV = 0, 805, 4010, 4015
ROW_VALUE, ROW_UP, ROW_HID, ROW_DOWN = 5615, 6425, 9625, 9735


def rows_from_flat(flat, base, pairs, buf):
    left = lax.broadcasted_iota(jnp.int32, (8, 128), 1) < 64

    def step(i, carry):
        t = [flat[pl.ds(base + 40 * i + k, 8, stride=5), :] for k in range(5)]
        r = [pltpu.roll(t[k], 64, 1) for k in range(2, 5)]
        even = (t[0], t[1], t[2])
        odd = (jnp.where(left, r[0], r[1]), jnp.where(left, r[1], r[2]), r[2])
        for k in range(3):
            buf.at[k][pl.ds(16 * i, 8, stride=2), :] = even[k]
            buf.at[k][pl.ds(16 * i + 1, 8, stride=2), :] = odd[k]
        return carry

    lax.fori_loop(0, -(-pairs // 8), step, 0)


def rows_to_flat(flat, base, pairs, buf):
    left = lax.broadcasted_iota(jnp.int32, (8, 128), 1) < 64

    def emit(i, size):
        even = [buf.at[k][pl.ds(16 * i, size, stride=2), :] for k in range(3)]
        odd = [buf.at[k][pl.ds(16 * i + 1, size, stride=2), :] for k in range(3)]
        r = [pltpu.roll(odd[k], 64, 1) for k in range(3)]
        lo = left[:size]
        t = (even[0], even[1], jnp.where(lo, even[2], r[0]),
             jnp.where(lo, r[0], r[1]), jnp.where(lo, r[1], r[2]))
        for k in range(5):
            flat[pl.ds(base + 40 * i + k, size, stride=5), :] = t[k]

    def step(i, carry):
        emit(i, 8)
        return carry

    lax.fori_loop(0, pairs // 8, step, 0)
    if pairs % 8:
        emit(pairs // 8, pairs % 8)


def buf_rows(buf, start, size):
    at = slice(start, start + size)
    return jnp.concatenate([buf[0, at], buf[1, at], buf[2, at][:, :64]], 1)


def put_rows(buf, start, value):
    at = slice(start, start + value.shape[0])
    buf[0, at] = value[:, :128]
    buf[1, at] = value[:, 128:256]
    buf[2, at, :64] = value[:, 256:]


def unpack_weights(
    shard_rows, wall, parts, psem, flat, buf, eye,
    wqt, wrt, wkvt, wot, wut, wdt, wq, wr, wkv, wo, wu, wd, vt, ht,
):
    groups = wall.shape[0] // 8
    loads = [
        pltpu.make_async_copy(wall.at[pl.ds(8 * g, 8)], parts.at[g % 2], psem.at[g % 2])
        for g in range(groups)
    ]
    loads[0].start()
    for g in range(groups):
        if g + 1 < groups:
            loads[g + 1].start()
        loads[g].wait()
        for k in range(8):
            at = shard_rows * (8 * g + k)
            flat[at : at + shard_rows, :] = parts[g % 2, k, :shard_rows].astype(F32)
    tail = shard_rows * wall.shape[0]
    flat[tail:, :] = jnp.zeros((flat.shape[0] - tail, 128), F32)
    vectors = {}

    def vector(slot, row):
        vectors[slot] = [buf[t, row : row + 1, :] for t in range(3)]

    def flip(w):
        return dot_nt(eye[: w.shape[1], : w.shape[1]], w).astype(BF16)

    rows_from_flat(flat, ROW_QUERY, 161, buf)
    wq[...] = buf_rows(buf, 2, C).astype(BF16)
    vector(V_NG, 0)
    vector(V_NB, 1)
    wqt[...] = flip(wq[...])
    rows_from_flat(flat, ROW_REDUCE, 641, buf)
    for k in range(4):
        wr[k] = buf_rows(buf, 1 + C * k, C).astype(BF16)
        wrt[k] = flip(wr[k])
    vector(V_QB, 0)
    vector(V_RB, 1281)
    rows_from_flat(flat, ROW_KEYS, 1, buf)
    vector(V_KG, 0)
    vector(V_KB, 1)
    for k in range(5):
        cols = flat[pl.ds(ROW_KV + k, C, stride=5), :]
        wkv[:, 128 * k : 128 * (k + 1)] = cols.astype(BF16)
        wkvt[128 * k : 128 * (k + 1), :] = flip(wkv[:, 128 * k : 128 * (k + 1)])
    rows_from_flat(flat, ROW_VALUE, 162, buf)
    wo[...] = buf_rows(buf, 1, C).astype(BF16)
    wot[...] = flip(wo[...])
    vector(V_VB, 0)
    vector(V_OB, 321)
    vector(V_MG, 322)
    vector(V_MB, 323)
    for k in range(10):
        cols = flat[pl.ds(ROW_UP + k, C, stride=10), :]
        wu[:, 128 * k : 128 * (k + 1)] = cols.astype(BF16)
        wut[128 * k : 128 * (k + 1), :] = flip(wu[:, 128 * k : 128 * (k + 1)])
    rows_from_flat(flat, ROW_DOWN, 641, buf)
    for k in range(5):
        at = slice(BLK * k, BLK * (k + 1))
        wd[at, :] = buf_rows(buf, BLK * k, BLK).astype(BF16)
        wdt[:, at] = flip(wd[at, :])
    vector(V_DB, 1280)
    for t in range(3):
        rows = jnp.concatenate([vectors[k][t] for k in range(11)] + [jnp.zeros((117, 128), F32)], 0)
        size = min(128, C - 128 * t)
        vt[128 * t : 128 * t + size, :] = rows.T[:size]
    for k in range(10):
        rows = flat[pl.ds(ROW_HID + k, 11, stride=10), :]
        rows = jnp.concatenate([rows, jnp.zeros((117, 128), F32)], 0)
        ht[128 * k : 128 * (k + 1), :] = rows.T


def pack_grads(shard_rows, flat, buf, gwq, gwr, gwkv, gwo, gwu, gwd, gv, gh):
    flat[ROW_DOWN + 3200 :, :] = jnp.zeros((flat.shape[0] - ROW_DOWN - 3200, 128), F32)

    def vector(slot, row):
        for t in range(3):
            size = min(128, C - 128 * t)
            part = gv[slot, 128 * t : 128 * t + size, :]
            if size < 128:
                part = jnp.concatenate([part, jnp.zeros((128 - size, 128), F32)], 0)
            buf[t, row : row + 1, :] = jnp.sum(part.T, 0, keepdims=True)

    put_rows(buf, 2, gwq[...])
    vector(V_NG, 0)
    vector(V_NB, 1)
    rows_to_flat(flat, ROW_QUERY, 161, buf)
    for k in range(4):
        put_rows(buf, 1 + C * k, gwr[k])
    vector(V_QB, 0)
    vector(V_RB, 1281)
    rows_to_flat(flat, ROW_REDUCE, 641, buf)
    vector(V_KG, 0)
    vector(V_KB, 1)
    rows_to_flat(flat, ROW_KEYS, 1, buf)
    for k in range(5):
        flat[pl.ds(ROW_KV + k, C, stride=5), :] = gwkv[:, 128 * k : 128 * (k + 1)]
    put_rows(buf, 1, gwo[...])
    vector(V_VB, 0)
    vector(V_OB, 321)
    vector(V_MG, 322)
    vector(V_MB, 323)
    rows_to_flat(flat, ROW_VALUE, 162, buf)
    for k in range(10):
        flat[pl.ds(ROW_UP + k, C, stride=10), :] = gwu[:, 128 * k : 128 * (k + 1)]
        for slot in range(11):
            part = gh[slot, 128 * k : 128 * (k + 1), :]
            at = ROW_HID + 10 * slot + k
            flat[at : at + 1, :] = jnp.sum(part.T, 0, keepdims=True)
    put_rows(buf, 0, gwd[...])
    vector(V_DB, 1280)
    for t in range(3):
        buf[t, 1281:1282, :] = jnp.zeros((1, 128), F32)
    rows_to_flat(flat, ROW_DOWN, 641, buf)
    half = ROW_DOWN + 3202
    flat[half : half + 1, 64:] = jnp.zeros((1, 64), F32)
    flat[half + 1 :, :] = jnp.zeros((flat.shape[0] - half - 1, 128), F32)


def image_kernel(
    shard_rows, work, x_ref, ct_ref, pool_ref, wall,
    out_ref, gin_ref, done_ref, gflat,
    wqt, wrt, wkvt, wot, wut, wdt, wq, wr, wkv, wo, wu, wd, vt, ht,
    gwq, gwr, gwkv, gwo, gwu, gwd, gv, gh,
    eye, sel, perm, flat, xp, xt, dzt, hgt, qt, attb, mt, yt, acc, dgt, dbt, dmt, dqt,
    rt, nt, kvt, kvc, kc, vc, dsb, dkvc, e_s, du_s, u_s, de_s, stat, stage, sem, parts, psem,
):
    slot = pl.program_id(0)
    own, live = work[1], work[2]
    lanes = lax.broadcasted_iota(jnp.int32, (8, 128), 1)
    low, high = lanes < 16, lanes >= 112

    @pl.when(slot == 0)
    def _():
        for ref in (gwq, gwr, gwkv, gwo, gwu, gwd, gv, gh):
            ref[...] = jnp.zeros(ref.shape, ref.dtype)
        r = lax.broadcasted_iota(jnp.int32, (C, C), 0)
        c = lax.broadcasted_iota(jnp.int32, (C, C), 1)
        eye[...] = (r == c).astype(F32).astype(BF16)
        r = lax.broadcasted_iota(jnp.int32, (KEYC, SLAB), 0)
        c = lax.broadcasted_iota(jnp.int32, (KEYC, SLAB), 1)
        i, j = c >> 4, c & 15
        hit = (r == i * HALF + j) & (i < HALF) & (j < HALF)
        sel[...] = hit.astype(F32).astype(BF16)
        unpack_weights(
            shard_rows, wall, parts, psem, flat, xp, eye,
            wqt, wrt, wkvt, wot, wut, wdt, wq, wr, wkv, wo, wu, wd, vt, ht,
        )
        for k in range(8):
            r = lax.broadcasted_iota(jnp.int32, (128, NTOK), 0) + 128 * k
            c = lax.broadcasted_iota(jnp.int32, (128, NTOK), 1)
            i, j = (r >> 4) & 15, r & 15
            want = (2 * i + (r >> 9)) * SIDE + 2 * j + ((r >> 8) & 1)
            hit = (c == want) & (i < HALF) & (j < HALF)
            perm[128 * k : 128 * (k + 1), :] = hit.astype(F32).astype(BF16)

    def take(src, dst):
        for k in range(4):
            ks = slice(SLAB * k, SLAB * (k + 1))
            dst[:, ks] = dot_nt(src[...], perm[ks, :]).astype(dst.dtype)

    def give(src, own_dst, part):
        acc[:, :NTOK] = dot_nn(src[...], perm[...])

        @pl.when(slot < own)
        def _():
            own_dst[0] = acc[:, :NTOK].astype(BF16)

        @pl.when(slot >= own)
        def _():
            done_ref[0, part] = acc[:, :NTOK].astype(BF16)

    @pl.when(slot < live)
    def _():
        @pl.when(slot < own)
        def _():
            take(x_ref.at[0], xt)
            take(ct_ref.at[0], dzt)

        @pl.when(slot >= own)
        def _():
            take(pool_ref.at[0, 0], xt)
            take(pool_ref.at[0, 1], dzt)

        mean, inv = ln_stats(xt, TOK)
        stat[0], stat[1] = mean, inv
        ln_apply(xt, hgt.at[0], mean, inv, vt, V_NG, V_NB)
        ht_ = hgt.at[0]
        qt[...] = (dot_nn(wqt[...], ht_[...]) + vt[:, V_QB : V_QB + 1]).astype(BF16)
        reduced = vt[:, V_RB : V_RB + 1]
        for k in range(4):
            reduced = reduced + dot_nn(wrt[k], ht_[:, SLAB * k : SLAB * (k + 1)])
        rt[...] = reduced
        kmean, kinv = ln_stats(rt, SLAB)
        stat[4, :, :SLAB], stat[5, :, :SLAB] = kmean, kinv
        ln_apply(rt, nt, kmean, kinv, vt, V_KG, V_KB)
        kvt[:C, :] = dot_nn(wkvt[:C, :], nt[...]).astype(BF16)
        kvt[C:, :] = (dot_nn(wkvt[C:, :], nt[...]) + vt[:, V_VB : V_VB + 1]).astype(BF16)
        kvc[...] = dot_nt(kvt[...], sel[...]).astype(BF16)

        def head_forward(h, carry):
            r = aligned(HEADSZ * h, HEADSZ)
            kc[h] = dot_nt(sel[...], kvt[pl.ds(r, HEADSZ), :]).astype(BF16)
            vc[h] = dot_nt(sel[...], kvt[pl.ds(aligned(C + r, HEADSZ), HEADSZ), :]).astype(BF16)
            scores = dot_nn(kc[h], qt[pl.ds(r, HEADSZ), :])
            for t in range(TOK // 128):
                flat[pl.ds(aligned((h * 8 + t) * KEYC, 8), KEYC), :] = scores[:, 128 * t : 128 * (t + 1)]

            def tile(t, carry):
                ls = pl.ds(aligned(128 * t, 128), 128)
                at = pl.ds(aligned((h * 8 + t) * KEYC, 8), KEYC)
                s = flat[at, :]
                rows = lax.broadcasted_iota(jnp.int32, (KEYC, 128), 0)
                s = jnp.where(rows < KEYS, s, -jnp.inf)
                top = jnp.max(s, 0, keepdims=True)
                p = jnp.exp2((s - top) * (LOG2E * HEADSZ**-0.5))
                p = p * (1.0 / jnp.sum(p, 0, keepdims=True))
                flat[at, :] = p
                attb[h, :, ls] = p.astype(BF16)
                return carry

            lax.fori_loop(0, TOK // 128, tile, 0)
            vt_h = kvc[pl.ds(aligned(C + r, HEADSZ), HEADSZ), :]
            mt[pl.ds(r, HEADSZ), :] = dot_nn(vt_h, attb[h]).astype(BF16)
            return carry

        lax.fori_loop(0, HEADS, head_forward, 0)
        yt[...] = xt[...] + (dot_nn(wot[...], mt[...]) + vt[:, V_OB : V_OB + 1])
        mean, inv = ln_stats(yt, TOK)
        stat[2], stat[3] = mean, inv
        ln_apply(yt, hgt.at[1], mean, inv, vt, V_MG, V_MB)
        gt = hgt.at[1]
        acc[...] = yt[...] + vt[:, V_DB : V_DB + 1]
        dgt[...] = jnp.zeros(dgt.shape, F32)
        lane16 = (lanes & 15) < HALF
        keep = (lane16, lane16 & (lanes < 96))

        def block(c, carry):
            span = pl.ds(aligned(BLK * c, BLK), BLK)
            e_s[...] = dot_nn(wut[span, :], gt[...])
            du_s[...] = dot_nn(wd[span, :], dzt[...])

            def group(i, carry):
                row = aligned(16 * i, 16)
                u_parts, de_parts = [], []
                for half in range(2):
                    r = aligned(row + 8 * half, 8)
                    chan = aligned(BLK * c + r, 8)
                    table = ht[pl.ds(chan, 8), :]
                    w = [jnp.broadcast_to(table[:, k : k + 1], (8, 128)) for k in range(11)]
                    taps = [w[1:4], w[4:7], w[7:10]]
                    flipped = [[w[9], w[8], w[7]], [w[6], w[5], w[4]], [w[3], w[2], w[1]]]
                    e = {}
                    for k in range(4):
                        e[k // 2, k % 2] = [
                            jnp.where(
                                keep[q],
                                e_s[pl.ds(r, 8), SLAB * k + 128 * q : SLAB * k + 128 * (q + 1)] + w[0],
                                0.0,
                            )
                            for q in range(2)
                        ]
                    views = side_views(e)
                    d = conv(views, taps, w[10], low, high)
                    dd, us = {}, []
                    for k in range(4):
                        out = []
                        for q in range(2):
                            value, slope = gelu_parts(d[k // 2, k % 2][q])
                            us.append(value)
                            out.append(
                                du_s[pl.ds(r, 8), SLAB * k + 128 * q : SLAB * k + 128 * (q + 1)] * slope
                            )
                        dd[k // 2, k % 2] = out
                    u_parts.append(us)
                    gsum = None
                    for k in range(4):
                        for q in range(2):
                            v = dd[k // 2, k % 2][q]
                            gsum = v if gsum is None else gsum + v
                    gh[10, pl.ds(chan, 8), :] += gsum
                    sums = tap_grads(views, dd, low, high)
                    for k in range(9):
                        gh[k + 1, pl.ds(chan, 8), :] += sums[k // 3][k % 3]
                    de = conv(side_views(dd), flipped, None, low, high)
                    des = [
                        jnp.where(keep[q], de[k // 2, k % 2][q], 0.0) for k in range(4) for q in range(2)
                    ]
                    de_parts.append(des)
                esums = [None, None]
                for k in range(8):
                    ls = slice(128 * k, 128 * (k + 1))
                    u_s[pl.ds(row, 16), ls] = jnp.concatenate(
                        [u_parts[0][k], u_parts[1][k]], 0
                    ).astype(BF16)
                    de16 = jnp.concatenate([de_parts[0][k], de_parts[1][k]], 0).astype(BF16)
                    de_s[pl.ds(row, 16), ls] = de16
                    wide = de16.astype(F32)
                    for half in range(2):
                        v = wide[8 * half : 8 * half + 8]
                        esums[half] = v if esums[half] is None else esums[half] + v
                chan = aligned(BLK * c + row, 16)
                gh[0, pl.ds(chan, 8), :] += esums[0]
                gh[0, pl.ds(aligned(chan + 8, 8), 8), :] += esums[1]
                return carry

            lax.fori_loop(0, BLK // 16, group, 0)
            acc[...] += dot_nn(wdt[:, span], u_s[...])
            dgt[...] += dot_nn(wu[:, span], de_s[...])
            gwd[span, :] += dot_nt(u_s[...], dzt[...])
            gwu[:, span] += dot_nt(gt[...], de_s[...])
            return carry

        lax.fori_loop(0, NBLK, block, 0)
        dbt[...] = acc[...].astype(BF16)
        give(dbt, out_ref, 0)

        def middle(row, parts):
            for half in range(2):
                r = aligned(row + 8 * half, 8)
                z = dzt[pl.ds(row, 16), :].astype(F32)[8 * half : 8 * half + 8]
                gv[V_DB, pl.ds(r, 8), :] += fold(z)
                parts[half] = parts[half] + z
            both = jnp.concatenate(parts, 0)
            acc[pl.ds(row, 16), :] = both
            low_part = both.astype(BF16)
            dbt[pl.ds(row, 16), :] = low_part
            wide = low_part.astype(F32)
            for half in range(2):
                r = aligned(row + 8 * half, 8)
                gv[V_OB, pl.ds(r, 8), :] += fold(wide[8 * half : 8 * half + 8])

        norm_back(dgt, yt, stat[2], stat[3], vt, V_MG, gv, V_MG, V_MB, middle)
        dmt[...] = dot_nn(wo[...], dbt[...]).astype(BF16)
        gwo[...] += dot_nt(mt[...], dbt[...])

        def head_backward(h, carry):
            r = aligned(HEADSZ * h, HEADSZ)
            hs = pl.ds(r, HEADSZ)
            da = e_s.at[pl.ds(0, KEYC), :]
            da[...] = dot_nn(vc[h], dmt[hs, :])

            def tile(t, carry):
                ls = pl.ds(aligned(128 * t, 128), 128)
                p = flat[pl.ds(aligned((h * 8 + t) * KEYC, 8), KEYC), :]
                g = da[:, ls]
                total = jnp.sum(p * g, 0, keepdims=True)
                dsb[:, ls] = (p * (g - total)).astype(BF16)
                return carry

            lax.fori_loop(0, TOK // 128, tile, 0)
            dkvc[pl.ds(aligned(C + r, HEADSZ), HEADSZ), :] = dot_nt(dmt[hs, :], attb[h]).astype(BF16)
            dqt[hs, :] = (dot_nn(kvc[hs, :], dsb[...]) * HEADSZ**-0.5).astype(BF16)
            dkvc[hs, :] = (dot_nt(qt[hs, :], dsb[...]) * HEADSZ**-0.5).astype(BF16)
            return carry

        lax.fori_loop(0, HEADS, head_backward, 0)
        kvt[...] = dot_nn(dkvc[...], sel[...]).astype(BF16)
        gwkv[...] += dot_nt(nt[...], kvt[...])
        dnt = dgt.at[:, pl.ds(0, SLAB)]
        dnt[...] = dot_nn(wkv[...], kvt[...])

        def vbias(i, carry):
            row = aligned(16 * i, 16)
            wide = kvt[pl.ds(aligned(C + row, 16), 16), :].astype(F32)
            gv[V_VB, pl.ds(row, 16), :] += fold(wide)
            return carry

        lax.fori_loop(0, C // 16, vbias, 0)

        def keys_out(row, parts):
            low_part = jnp.concatenate(parts, 0).astype(BF16)
            nt[pl.ds(row, 16), :] = low_part
            gv[V_RB, pl.ds(row, 16), :] += fold(low_part.astype(F32))

        norm_back(
            dnt, rt, stat[4, :, :SLAB], stat[5, :, :SLAB], vt, V_KG, gv, V_KG, V_KB, keys_out
        )
        for k in range(4):
            ls = slice(SLAB * k, SLAB * (k + 1))
            gwr[k] += dot_nt(ht_[:, ls], nt[...])
            dgt[:, ls] = dot_nn(wq[...], dqt[:, ls]) + dot_nn(wr[k], nt[...])
        gwq[...] += dot_nt(ht_[...], dqt[...])

        def qbias(i, carry):
            row = aligned(16 * i, 16)
            gv[V_QB, pl.ds(row, 16), :] += fold(dqt[pl.ds(row, 16), :].astype(F32))
            return carry

        lax.fori_loop(0, C // 16, qbias, 0)

        def final(row, parts):
            both = jnp.concatenate(parts, 0) + acc[pl.ds(row, 16), :]
            dbt[pl.ds(row, 16), :] = both.astype(BF16)

        norm_back(dgt, xt, stat[0], stat[1], vt, V_NG, gv, V_NG, V_NB, final)
        give(dbt, gin_ref, 1)

    @pl.when(slot == pl.num_programs(0) - 1)
    def _():
        pack_grads(shard_rows, flat, xp, gwq, gwr, gwkv, gwo, gwu, gwd, gv, gh)
        copies = []
        for k in range(gflat.shape[0]):
            if k >= 2:
                copies[k - 2].wait()
            stage[k % 2] = flat[shard_rows * k : shard_rows * k + gflat.shape[1], :]
            copies.append(pltpu.make_async_copy(stage.at[k % 2], gflat.at[k], sem.at[k % 2]))
            copies[k].start()
        copies[-2].wait()
        copies[-1].wait()


def run_images(work, images, cotangent, pool, gathered, shard_rows):
    count, padded = gathered.shape[:2]
    item = pl.BlockSpec(
        (1, C, NTOK), lambda s, w: (jnp.maximum(jnp.minimum(s, w[1] - 1), 0), 0, 0)
    )
    foreign = pl.BlockSpec(
        (1, 2, C, NTOK),
        lambda s, w: (w[3 + jnp.clip(jnp.minimum(s, w[2] - 1) - w[1], 0, POOL - 1)], 0, 0, 0),
    )
    once = pl.BlockSpec(foreign.block_shape, foreign.index_map, pipeline_mode=pl.Buffered(1))
    anywhere = pl.BlockSpec(memory_space=pl.ANY)
    wide = lambda *dims: pltpu.VMEM(dims, F32)
    thin = lambda *dims: pltpu.VMEM(dims, BF16)
    flat_rows = -(-(count * shard_rows + 24) // 8) * 8
    scratch = [
        thin(C, C), thin(4, C, C), thin(2 * C, C), thin(C, C), thin(HID, C), thin(C, HID),
        thin(C, C), thin(4, C, C), thin(C, 2 * C), thin(C, C), thin(C, HID), thin(HID, C),
        wide(C, 128), wide(HID, 128),
        wide(C, C), wide(4, C, C), wide(C, 2 * C), wide(C, C), wide(C, HID), wide(HID, C),
        wide(11, C, 128), wide(11, HID, 128),
        thin(C, C), thin(KEYC, SLAB), thin(TOK, NTOK), wide(flat_rows, 128), wide(3, 1296, 128),
        wide(C, TOK), thin(C, TOK), thin(2, C, TOK), thin(C, TOK),
        thin(HEADS, KEYC, TOK), thin(C, TOK), wide(C, TOK),
        wide(C, TOK), wide(C, TOK), thin(C, TOK), thin(C, TOK), thin(C, TOK),
        wide(C, SLAB), thin(C, SLAB), thin(2 * C, SLAB), thin(2 * C, KEYC),
        thin(HEADS, KEYC, HEADSZ), thin(HEADS, KEYC, HEADSZ), thin(KEYC, TOK), thin(2 * C, KEYC),
        wide(BLK, TOK), wide(BLK, TOK), thin(BLK, TOK), thin(BLK, TOK), wide(6, 8, TOK),
        wide(2, padded, 128), pltpu.SemaphoreType.DMA((2,)),
        thin(2, 8, padded, 128), pltpu.SemaphoreType.DMA((2,)),
    ]
    call = pl.pallas_call(
        functools.partial(image_kernel, shard_rows),
        out_shape=[jax.ShapeDtypeStruct(images.shape, BF16)] * 2
        + [jax.ShapeDtypeStruct(pool.shape, BF16), jax.ShapeDtypeStruct((count, padded, 128), F32)],
        grid_spec=pltpu.PrefetchScalarGridSpec(
            num_scalar_prefetch=1,
            grid=(CAP + MOVES,),
            in_specs=[
                item, item, once,
                anywhere,
            ],
            out_specs=[item, item, foreign, anywhere],
            scratch_shapes=scratch,
        ),
        compiler_params=pltpu.CompilerParams(
            dimension_semantics=("arbitrary",), vmem_limit_bytes=67043328
        ),
        name="image_block",
    )
    return call(work, images, cotangent, pool, gathered)


MESH = pl.DeviceIdType.MESH


class Place:
    def __init__(self, dims):
        self.dp, self.fsdp = dims
        self.ny, self.nz = self.dp // 2, self.fsdp // 2
        dp, fsdp = lax.axis_index("dp"), lax.axis_index("fsdp")
        self.y, self.c = dp // 2, dp % 2
        self.z, self.x = fsdp // 2, fsdp % 2
        self.offsets = [(dy, dx) for dy in range(self.ny) for dx in range(2)]

    def at(self, dy=0, dc=0, dz=0, dx=0):
        y, c = (self.y + dy) % self.ny, (self.c + dc) % 2
        z, x = (self.z + dz) % self.nz, (self.x + dx) % 2
        return y * 2 + c, z * 2 + x

    def index(self, **move):
        dp, fsdp = self.at(**move)
        return dp * self.fsdp + fsdp

    def target(self, **move):
        dp, fsdp = self.at(**move)
        return {"dp": dp, "fsdp": fsdp}

    def peers(self):
        moves = [dict(dz=k) for k in range(1, self.nz)]
        moves += [dict(dy=dy, dx=dx) for dy, dx in self.offsets[1:]]
        return moves + [dict(dc=1)]

    def enter(self):
        barrier = pltpu.get_barrier_semaphore()
        moves = self.peers()
        for move in moves:
            pl.semaphore_signal(barrier, inc=1, device_id=self.target(**move), device_id_type=MESH)
        pl.semaphore_wait(barrier, len(moves))


def remote(src, dst, send, recv, target):
    return pltpu.make_async_remote_copy(
        src_ref=src, dst_ref=dst, send_sem=send, recv_sem=recv, device_id=target, device_id_type=MESH
    )


def gather_kernel(dims, low_ref, out_ref, send, recv):
    p = Place(dims)
    p.enter()
    started = []

    def push(src, slot, **move):
        cp = remote(src, out_ref.at[slot], send.at[len(started)], recv.at[slot], p.target(**move))
        cp.start()
        started.append(cp)

    def arrived(slot):
        remote(low_ref, out_ref.at[slot], send.at[0], recv.at[slot], p.target(dc=1)).wait_recv()

    mine = p.index()
    for dz in range(1, p.nz):
        push(low_ref, mine, dz=dz)
    out_ref[mine] = low_ref[...]
    for dz in range(p.nz):
        slot = p.index(dz=dz)
        if dz:
            arrived(slot)
        src = out_ref.at[slot] if dz else low_ref
        for dy, dx in p.offsets[1:]:
            push(src, slot, dy=dy, dx=dx)
        push(src, slot, dc=1)
    for dz in range(p.nz):
        for dy, dx in p.offsets[1:]:
            slot = p.index(dz=dz, dy=dy, dx=dx)
            arrived(slot)
            push(out_ref.at[slot], slot, dc=1)
    for dz in range(p.nz):
        for dy, dx in p.offsets:
            arrived(p.index(dz=dz, dy=dy, dx=dx, dc=1))
    for cp in started:
        cp.wait_send()


def all_weights(dims, low):
    count = dims[0] * dims[1]
    ny, nz = dims[0] // 2, dims[1] // 2
    sends = nz - 1 + nz * 2 * ny + nz * (2 * ny - 1)
    vmem = pl.BlockSpec(memory_space=pltpu.VMEM)
    return pl.pallas_call(
        functools.partial(gather_kernel, dims),
        out_shape=jax.ShapeDtypeStruct((count,) + low.shape, low.dtype),
        in_specs=[vmem],
        out_specs=vmem,
        scratch_shapes=[pltpu.SemaphoreType.DMA((sends,)), pltpu.SemaphoreType.DMA((count,))],
        compiler_params=pltpu.CompilerParams(
            collective_id=0, has_side_effects=True, vmem_limit_bytes=32 * 1024 * 1024
        ),
        name="weights_gather",
    )(low)


MOVES = 4
RELAYS = 3
POOL = MOVES + RELAYS


@functools.lru_cache(maxsize=None)
def routing(ny, nz, variants=8):
    chips = ny * nz * 2
    at = lambda y, z, x: (y * nz + z) * 2 + x
    edges = []
    for y in range(ny):
        for z in range(nz):
            edges.append((at(y, z, 0), at(y, z, 1), 0, 0))
            for x in range(2):
                if y % 2 == 0 and y + 1 < ny:
                    edges.append((at(y, z, x), at(y + 1, z, x), 1, 1))
                if z < nz - 1:
                    edges.append((at(y, z, x), at(y, z + 1, x), 2, 3))
    count = len(edges)
    incidence = np.zeros((count, chips))
    sides = np.zeros((MOVES, chips, count), np.float32)
    for e, (u, v, du, dv) in enumerate(edges):
        incidence[e, u], incidence[e, v] = 1, -1
        sides[du, u, e], sides[dv, v, e] = 1, -1
    ideal = incidence @ np.linalg.pinv(incidence.T @ incidence)
    rng = np.random.default_rng(7)
    guess, exact, fix = [], [], []
    for variant in range(variants):
        order = rng.permutation(count)
        root = list(range(chips))

        def find(a):
            while root[a] != a:
                a = root[a]
            return a

        tree = []
        for e in order:
            a, b = find(edges[e][0]), find(edges[e][1])
            if a != b:
                root[a] = b
                tree.append(e)
        others = [e for e in range(count) if e not in tree]
        near = {k: [] for k in range(chips)}
        for e in tree:
            near[edges[e][0]].append((edges[e][1], e))
            near[edges[e][1]].append((edges[e][0], e))
        a_mat, b_mat = np.zeros((count, chips)), np.zeros((count, count))
        for e in tree:
            side, todo = {edges[e][0]}, [edges[e][0]]
            while todo:
                for b, via in near[todo.pop()]:
                    if via != e and b not in side:
                        side.add(b)
                        todo.append(b)
            a_mat[e, list(side)] = 1
            for q in others:
                b_mat[e, q] = (edges[q][1] in side) * 1 - (edges[q][0] in side) * 1
        g_mat = np.zeros((count, chips))
        for q in others:
            b_mat[q, q] = 1
            g_mat[q] = ideal[q]
        guess.append(g_mat)
        exact.append(a_mat)
        fix.append(b_mat)
    stack = lambda items: np.stack(items).astype(np.float32)
    return stack(guess), stack(exact), stack(fix), sides


def plan(dims, counts):
    ny, nz = dims[0] // 2, dims[1] // 2
    guess, exact, fix, sides = routing(ny, nz)
    chips = ny * nz * 2
    c = counts.reshape(ny, 2, nz, 2).transpose(0, 2, 3, 1).reshape(chips, 2)
    total = jnp.sum(c, 1).astype(F32)
    excess = total - jnp.sum(total) / chips
    high = lax.Precision.HIGHEST
    near = jnp.round(jnp.einsum("tek,k->te", guess, excess, precision=high))
    flow = jnp.einsum("tek,k->te", exact, excess, precision=high)
    flow = jnp.round(flow + jnp.einsum("teq,tq->te", fix, near, precision=high))
    cost = jnp.sum(jnp.maximum(jnp.abs(flow) - 2.0, 0.0) + 0.001 * jnp.abs(flow), 1)
    best = flow[jnp.argmin(cost)]
    out = jnp.clip(jnp.einsum("dke,e->dk", sides, best, precision=high), 0, 2).astype(jnp.int32)
    left = [c[:, 0], c[:, 1]]
    takes, order = {}, {}
    for d in (2, 3, 0, 1):
        bigger = left[0] >= left[1]
        both, one = out[d] == 2, out[d] == 1
        t = [
            (both | (one & bigger)) & (left[0] > 0),
            (both | (one & ~bigger)) & (left[1] > 0),
        ]
        t = [v.astype(jnp.int32) for v in t]
        left = [left[0] - t[0], left[1] - t[1]]
        takes[d] = jnp.stack(t, 1)
        order[d] = jnp.stack(left, 1)
    kept = jnp.stack(left, 1)
    grid = lambda v: v.reshape(ny, nz, 2, 2)
    zero = jnp.zeros((ny, 1, 2, 2), jnp.int32)
    got = [
        grid(takes[0])[:, :, ::-1],
        grid(takes[1]).reshape(ny // 2, 2, nz, 2, 2)[:, ::-1].reshape(ny, nz, 2, 2),
        jnp.concatenate([zero, grid(takes[2])[:, :-1]], 1),
        jnp.concatenate([grid(takes[3])[:, 1:], zero], 1),
    ]
    got = [v.reshape(chips, 2) for v in got]
    load = kept + got[0] + got[1] + got[2] + got[3]
    give = jnp.clip((load - load[:, ::-1]) // 2, 0, RELAYS)
    take_in = give[:, ::-1]
    dp, fsdp = lax.axis_index("dp"), lax.axis_index("fsdp")
    me = ((dp // 2) * nz + fsdp // 2) * 2 + fsdp % 2
    pack = jnp.stack(
        [c, kept, load, give, take_in]
        + [takes[d] for d in range(MOVES)]
        + [order[d] for d in range(MOVES)]
        + got,
        0,
    )
    mine = lax.dynamic_slice(pack, (0, me, dp % 2), (pack.shape[0], 1, 1)).reshape(-1)
    have, keep, items, send, accept = (mine[k] for k in range(5))
    taken, place, came = mine[5:9], mine[9:13], mine[13:17]
    stay = items - send
    send_index = jnp.clip(place, 0, CAP - 1)
    rank = keep + jnp.cumsum(came) - came
    entry = stay + jnp.arange(RELAYS)
    from_move = jnp.sum(
        jnp.where((rank[None] == entry[:, None]) & (came[None] > 0), jnp.arange(MOVES)[None], 0), 1
    )
    relay_index = jnp.where(entry < keep, jnp.clip(entry, 0, CAP - 1), CAP + from_move)
    own = jnp.minimum(keep, stay)
    item = own + jnp.arange(POOL)
    from_item = jnp.sum(
        jnp.where((rank[None] == item[:, None]) & (came[None] > 0), jnp.arange(MOVES)[None], 0), 1
    )
    foreign = jnp.where(item < stay, from_item, jnp.clip(MOVES + item - stay, 0, POOL - 1))
    bring = jnp.concatenate([send_index, relay_index]).astype(jnp.int32)
    work = jnp.concatenate(
        [jnp.stack([jnp.maximum(stay + accept, 1), own, stay + accept]), foreign]
    ).astype(jnp.int32)
    back = jnp.where(rank < stay, jnp.arange(MOVES), POOL + jnp.clip(rank - stay, 0, RELAYS - 1))
    slot = jnp.arange(CAP)
    sent = jnp.sum(
        jnp.where((place[None] == slot[:, None]) & (taken[None] > 0), jnp.arange(MOVES)[None], 0), 1
    )
    source = jnp.where(
        slot >= keep,
        CAP + sent,
        jnp.where(slot >= stay, CAP + MOVES + jnp.clip(slot - stay, 0, RELAYS - 1), slot),
    )
    final = jnp.concatenate([own[None], source, (slot < have).astype(jnp.int32)])
    return bring, work, back.astype(jnp.int32), final.astype(jnp.int32)


def move_targets(p):
    return ((p.target(dx=1), None), (p.target(dy=1 - 2 * (p.y % 2)), None),
            (p.target(dz=1), p.z < p.nz - 1), (p.target(dz=-1), p.z > 0))


def guarded(cond, action):
    if cond is None:
        action()
    else:
        pl.when(cond)(action)


def greet(p):
    barrier = pltpu.get_barrier_semaphore()

    def signal(target):
        pl.semaphore_signal(barrier, inc=1, device_id=target, device_id_type=MESH)

    for target, cond in move_targets(p):
        guarded(cond, lambda target=target: signal(target))
    signal(p.target(dc=1))
    inner = (p.z < p.nz - 1).astype(jnp.int32) + (p.z > 0).astype(jnp.int32)
    pl.semaphore_wait(barrier, 3 + inner)


def bring_kernel(dims, tbl, x_ref, ct_ref, pool, stage, landed, relay, msem, rsem):
    p = Place(dims)
    greet(p)
    targets = move_targets(p)
    arriving = (None, None, p.z > 0, p.z < p.nz - 1)
    for d in range(MOVES):
        stage[d, 0] = x_ref[tbl[d]]
        stage[d, 1] = ct_ref[tbl[d]]
    copies = [
        remote(stage.at[d], landed.at[d], msem.at[0, d], msem.at[1, d], targets[d][0])
        for d in range(MOVES)
    ]
    for d in range(MOVES):
        guarded(targets[d][1], copies[d].start)
    for d in range(MOVES):
        guarded(arriving[d], copies[d].wait_recv)
    for j in range(RELAYS):
        pick = tbl[MOVES + j]
        own, got = jnp.minimum(pick, CAP - 1), jnp.maximum(pick - CAP, 0)
        for part, ref in enumerate((x_ref, ct_ref)):
            relay[j, part] = jnp.where(pick < CAP, ref[own], landed[got, part])
    passed = [
        remote(relay.at[j], pool.at[MOVES + j], rsem.at[0, j], rsem.at[1, j], p.target(dc=1))
        for j in range(RELAYS)
    ]
    for cp in passed:
        cp.start()
    for d in range(MOVES):
        pool[d] = landed[d]
    for cp in passed:
        cp.wait_recv()
    for cp in passed:
        cp.wait_send()
    for d in range(MOVES):
        guarded(targets[d][1], copies[d].wait_send)


def bring_images(dims, table, images, cotangent):
    vmem = pl.BlockSpec(memory_space=pltpu.VMEM)
    item = (2,) + images.shape[1:]
    dma = pltpu.SemaphoreType.DMA
    return pl.pallas_call(
        functools.partial(bring_kernel, dims),
        out_shape=jax.ShapeDtypeStruct((POOL,) + item, BF16),
        in_specs=[pl.BlockSpec(memory_space=pltpu.SMEM), vmem, vmem],
        out_specs=vmem,
        scratch_shapes=[
            pltpu.VMEM((MOVES,) + item, BF16), pltpu.VMEM((MOVES,) + item, BF16),
            pltpu.VMEM((RELAYS,) + item, BF16), dma((2, MOVES)), dma((2, RELAYS)),
        ],
        compiler_params=pltpu.CompilerParams(
            collective_id=2, has_side_effects=True, vmem_limit_bytes=56 * 1024 * 1024
        ),
        name="bring_images",
    )(table, images, cotangent)


def settle_kernel(
    dims, tbl, g_ref, done, sum_ref, back, core,
    stage, mine, other, sx, rx, sz, rz, csem, bsem, lsem, gsem, xsem, zsem,
):
    p = Place(dims)
    p.enter()
    n_xy = len(p.offsets)
    order = list(range(1, p.nz)) + [0]
    targets = move_targets(p)
    routes = ((targets[0][0], None), (targets[1][0], None), targets[3], targets[2])
    arriving = (None, None, targets[2][1], targets[3][1])
    passed = [
        remote(done.at[MOVES + j], core.at[j], csem.at[0, j], csem.at[1, j], p.target(dc=1))
        for j in range(RELAYS)
    ]
    for cp in passed:
        cp.start()
    local, cross = {}, {}
    for dz in order:
        for k, (dy, dx) in enumerate(p.offsets):
            cp = remote(
                g_ref.at[p.index(dy=dy, dx=dx, dz=dz, dc=1)], other.at[dz, k],
                gsem.at[0, dz, k], gsem.at[1, dz, k], p.target(dc=1),
            )
            cp.start()
            cross[dz, k] = cp
            cp = pltpu.make_async_copy(
                g_ref.at[p.index(dy=dy, dx=dx, dz=dz)], mine.at[dz, k], lsem.at[dz, k]
            )
            cp.start()
            local[dz, k] = cp
    for cp in passed:
        cp.wait_recv()
    for d in range(MOVES):
        pick = tbl[d]
        here, there = jnp.minimum(pick, POOL - 1), jnp.maximum(pick - POOL, 0)
        for part in range(2):
            stage[d, part] = jnp.where(pick < POOL, done[here, part], core[there, part])
    copies = [
        remote(stage.at[d], back.at[d], bsem.at[0, d], bsem.at[1, d], routes[d][0])
        for d in range(MOVES)
    ]
    planar = {}
    waiting = None
    for step, dz in enumerate(order):
        for k in list(range(1, n_xy)) + [0]:
            dy, dx = p.offsets[k]
            local[dz, k].wait()
            cross[dz, k].wait_recv()
            total = mine[dz, k] + other[dz, k]
            if k == 0:
                mine[dz, 0] = total
            else:
                sx[dz, k - 1] = total.astype(BF16)
            if waiting is not None:
                waiting.start()
                waiting = None
            if k:
                waiting = remote(
                    sx.at[dz, k - 1], rx.at[dz, k - 1],
                    xsem.at[0, dz, k - 1], xsem.at[1, dz, k - 1], p.target(dy=dy, dx=dx),
                )
                planar[dz, k] = waiting
    for d in range(MOVES):
        guarded(routes[d][1], copies[d].start)
    final = None
    lines = {}
    for dz in order:
        total = mine[dz, 0]
        for k in range(1, n_xy):
            planar[dz, k].wait_recv()
            total = total + rx[dz, k - 1].astype(F32)
        if dz:
            sz[dz - 1] = total.astype(BF16)
        else:
            final = total
        if waiting is not None:
            waiting.start()
            waiting = None
        if dz:
            waiting = remote(
                sz.at[dz - 1], rz.at[dz - 1], zsem.at[0, dz - 1], zsem.at[1, dz - 1], p.target(dz=dz)
            )
            lines[dz] = waiting
    for dz in range(1, p.nz):
        lines[dz].wait_recv()
        final = final + rz[dz - 1].astype(F32)
    sum_ref[...] = final
    for d in range(MOVES):
        guarded(arriving[d], copies[d].wait_recv)
    for group in (cross, planar, lines):
        for cp in group.values():
            cp.wait_send()
    for cp in passed:
        cp.wait_send()
    for d in range(MOVES):
        guarded(routes[d][1], copies[d].wait_send)


def settle(dims, table, terms, done):
    ny, nz = dims[0] // 2, dims[1] // 2
    n_xy = 2 * ny
    rows = terms.shape[1]
    item = done.shape[1:]
    dma = pltpu.SemaphoreType.DMA
    vmem = pl.BlockSpec(memory_space=pltpu.VMEM)
    return pl.pallas_call(
        functools.partial(settle_kernel, dims),
        out_shape=[
            jax.ShapeDtypeStruct((rows, 128), F32),
            jax.ShapeDtypeStruct((MOVES,) + item, BF16),
            jax.ShapeDtypeStruct((RELAYS,) + item, BF16),
        ],
        in_specs=[
            pl.BlockSpec(memory_space=pltpu.SMEM), pl.BlockSpec(memory_space=pl.ANY), vmem,
        ],
        out_specs=[vmem, vmem, vmem],
        scratch_shapes=[
            pltpu.VMEM((MOVES,) + item, BF16),
            pltpu.VMEM((nz, n_xy, rows, 128), F32),
            pltpu.VMEM((nz, n_xy, rows, 128), F32),
            pltpu.VMEM((nz, n_xy - 1, rows, 128), BF16),
            pltpu.VMEM((nz, n_xy - 1, rows, 128), BF16),
            pltpu.VMEM((nz - 1, rows, 128), BF16),
            pltpu.VMEM((nz - 1, rows, 128), BF16),
            dma((2, RELAYS)), dma((2, MOVES)),
            dma((nz, n_xy)), dma((2, nz, n_xy)), dma((2, nz, n_xy - 1)), dma((2, nz - 1)),
        ],
        compiler_params=pltpu.CompilerParams(
            collective_id=1, has_side_effects=True, vmem_limit_bytes=60 * 1024 * 1024
        ),
        name="settle",
    )(table, terms, done)


def merge_kernel(tbl, own_out, own_grad, back, core, out_ref, gin_ref):
    slot = jnp.clip(jnp.maximum(pl.program_id(0), tbl[0]), 0, CAP - 1)
    pick, live = tbl[1 + slot], tbl[1 + CAP + slot]

    def put(first, second):
        out_ref[0] = first
        gin_ref[0] = second

    @pl.when(live == 0)
    def _():
        put(jnp.zeros(out_ref.shape[1:], BF16), jnp.zeros(out_ref.shape[1:], BF16))

    @pl.when((live > 0) & (pick < CAP))
    def _():
        put(own_out[0], own_grad[0])

    @pl.when((live > 0) & (pick >= CAP) & (pick < CAP + MOVES))
    def _():
        put(back[0, 0], back[0, 1])

    @pl.when((live > 0) & (pick >= CAP + MOVES))
    def _():
        put(core[0, 0], core[0, 1])


def merge(table, own_out, own_grad, back, core):
    block = (1,) + own_out.shape[1:]
    place = lambda s, t: jnp.clip(jnp.maximum(s, t[0]), 0, CAP - 1)
    own = pl.BlockSpec(block, lambda s, t: (place(s, t), 0, 0))
    pair = (1, 2) + own_out.shape[1:]
    source = lambda s, t: t[1 + place(s, t)]
    moved = pl.BlockSpec(pair, lambda s, t: (jnp.clip(source(s, t) - CAP, 0, MOVES - 1), 0, 0, 0))
    relayed = pl.BlockSpec(
        pair, lambda s, t: (jnp.clip(source(s, t) - CAP - MOVES, 0, RELAYS - 1), 0, 0, 0)
    )
    return pl.pallas_call(
        merge_kernel,
        out_shape=[jax.ShapeDtypeStruct(own_out.shape, BF16)] * 2,
        grid_spec=pltpu.PrefetchScalarGridSpec(
            num_scalar_prefetch=1,
            grid=(CAP,),
            in_specs=[own, own, moved, relayed],
            out_specs=[own, own],
        ),
        input_output_aliases={1: 0, 2: 1},
        compiler_params=pltpu.CompilerParams(dimension_semantics=("arbitrary",)),
        name="merge",
    )(table, own_out, own_grad, back, core)


def body(images, counts, cotangent, master, first_moment, second_moment, average):
    dims = (lax.axis_size("dp"), lax.axis_size("fsdp"))
    shard_rows = master.shape[0] // 128
    padded = -(-(shard_rows + 1) // 16) * 16
    low = jnp.concatenate(
        [
            master.reshape(shard_rows, 128).astype(BF16),
            jnp.broadcast_to(counts.astype(BF16)[:, None], (1, 128)),
            jnp.zeros((padded - shard_rows - 1, 128), BF16),
        ],
        0,
    )
    gathered = all_weights(dims, low)
    bring, work, home, final = plan(dims, gathered[:, shard_rows, 0].astype(jnp.int32))
    flip = lambda v: jnp.swapaxes(v, 1, 2)
    images, cotangent = flip(images), flip(cotangent)
    pool = bring_images(dims, bring, images, cotangent)
    own_out, own_grad, done, terms = run_images(
        work, images, cotangent, pool, gathered, shard_rows
    )
    totals, back, core = settle(dims, home, terms, done)
    output_images, grad_images = merge(final, own_out, own_grad, back, core)
    output_images, grad_images = flip(output_images), flip(grad_images)
    grads = totals[:shard_rows].reshape(-1)
    new_first = beta_first * first_moment + (1.0 - beta_first) * grads
    new_second = beta_second * second_moment + (1.0 - beta_second) * grads * grads
    fix_first = 1.0 - beta_first**STEP
    fix_second = 1.0 - beta_second**STEP
    step_size = (
        new_first / fix_first / (jnp.sqrt(new_second / fix_second) + adam_eps)
        + weight_decay * master
    )
    new_master = master - learn_rate * step_size
    new_average = ema_keep * average + (1.0 - ema_keep) * new_master
    return (
        grads,
        new_first,
        new_second,
        new_master,
        new_average,
        new_master.astype(jnp.bfloat16),
        output_images,
        grad_images,
    )


def solution(mesh):
    return jax.shard_map(
        body,
        mesh=mesh,
        in_specs=(
            P(("dp", "fsdp"), None, None),
            P(("dp", "fsdp")),
            P(("dp", "fsdp"), None, None),
            P(("dp", "fsdp")),
            P(("dp", "fsdp")),
            P(("dp", "fsdp")),
            P(("dp", "fsdp")),
        ),
        out_specs=(
            P(("dp", "fsdp")),
            P(("dp", "fsdp")),
            P(("dp", "fsdp")),
            P(("dp", "fsdp")),
            P(("dp", "fsdp")),
            P(("dp", "fsdp")),
            P(("dp", "fsdp"), None, None),
            P(("dp", "fsdp"), None, None),
        ),
        check_vma=False,
    )
```
